32 devices in a mesh: frames: 8 (over z, x), rows: 4 (over y, core).
Axes of the slice: x: 2, y: 2, z: 4, core: 2. Of those that a mesh axis runs over, the one named last changes fastest.
Arguments:
- video: bfloat16 [8, 32, 160, 512], P('frames', 'rows'), may hold values from -6 to 6
- norm1_gain: float32 [512], replicated, may hold values from 0.25 to 1.75
- norm1_shift: float32 [512], replicated, may hold values from -1.75 to 1.75
- conv1_weight: bfloat16 [3, 3, 512, 512], replicated, may hold values from -0.09375 to 0.09375
- conv1_bias: float32 [512], replicated, may hold values from -1.75 to 1.75
- norm2_gain: float32 [512], replicated, may hold values from 0.25 to 1.75
- norm2_shift: float32 [512], replicated, may hold values from -1.75 to 1.75
- conv2_weight: bfloat16 [3, 3, 512, 512], replicated, may hold values from -0.09375 to 0.09375
- conv2_bias: float32 [512], replicated, may hold values from -1.75 to 1.75
- out_gain: float32 [512], replicated, may hold values from 0.25 to 1.75
- out_shift: float32 [512], replicated, may hold values from -1.75 to 1.75
- out_weight: bfloat16 [3, 3, 512, 8], replicated, may hold values from -0.09375 to 0.09375
- out_bias: float32 [8], replicated, may hold values from -1.75 to 1.75
- quant_weight: float32 [8, 4], replicated, may hold values from -2 to 2
- quant_bias: float32 [4], replicated, may hold values from -1.75 to 1.75
- time_in_weight: bfloat16 [3, 3, 3, 4, 128], replicated, may hold values from -0.625 to 0.625
- time_in_bias: float32 [128], replicated, may hold values from -1.75 to 1.75
- tnorm1_gain: float32 [128], replicated, may hold values from 0.25 to 1.75
- tnorm1_shift: float32 [128], replicated, may hold values from -1.75 to 1.75
- time1_weight: bfloat16 [3, 3, 3, 128, 128], replicated, may hold values from -0.109375 to 0.109375
- tnorm2_gain: float32 [128], replicated, may hold values from 0.25 to 1.75
- tnorm2_shift: float32 [128], replicated, may hold values from -1.75 to 1.75
- time2_weight: bfloat16 [3, 3, 3, 128, 128], replicated, may hold values from -0.109375 to 0.109375
- time2_bias: float32 [128], replicated, may hold values from -1.75 to 1.75
Outputs:
- features: bfloat16 [8, 32, 160, 128], P('frames', 'rows')
The draws below stay inside these ranges and needn't reach their ends.
All inputs are finite; a program needn't handle non-finite values.
Results may differ from the reference program's by a relative error of at most 0.01.
Values may be sent and summed in bfloat16 or wider, within the bound.
No kernel may reach another device: no remote copies, remote signals or barrier semaphores. Data moves between devices by JAX's collectives and lax.ppermute only.
A program may use at most 64 MiB of HBM per device.

```python
import jax
import jax.numpy as jnp
from jax import lax

CH = 512
LATENT = 4
TCH = 128
GROUPS = 32
WIDTH = 160
MOMENTS = 8
FRAMES = 8
HEIGHT = 32


def level_of(own_key, shape, split, least, top_value):
    gain = 1.0
    for axis_at, blocks in split:
        heights = jax.random.uniform(jax.random.fold_in(jax.random.fold_in(own_key, 6), axis_at), (blocks,), jnp.float32, least / len(split), top_value / len(split))
        gain = gain * jnp.repeat(jnp.exp(heights), shape[axis_at] // blocks).reshape((-1,) + (1,) * (len(shape) - 1 - axis_at))
    return gain


def scatter_about(key, dims, width, most, pieces=(), kind=jnp.bfloat16):
    values = width * jax.random.normal(key, dims, jnp.float32)
    if pieces:
        values = values * level_of(key, dims, pieces, -0.22, 0.18)
    return jnp.clip(values, -most, most).astype(kind)


def setup_inputs(seed: int = 0) -> dict:
    splits = jax.random.split(jax.random.key(seed), 25)
    return {
        "video": scatter_about(splits[0], (FRAMES, HEIGHT, WIDTH, CH), 1.0, 6.0, ((0, 8), (1, 4))),
        "norm1_gain": jnp.clip(1.0 + 0.15 * jax.random.normal(splits[1], (CH,), jnp.float32), 0.25, 1.75),
        "norm1_shift": scatter_about(splits[2], (CH,), 0.3, 1.75, (), jnp.float32),
        "conv1_weight": scatter_about(splits[3], (3, 3, CH, CH), (9 * CH) ** -0.5, 0.09375),
        "conv1_bias": scatter_about(splits[4], (CH,), 0.3, 1.75, (), jnp.float32),
        "norm2_gain": jnp.clip(1.0 + 0.15 * jax.random.normal(splits[5], (CH,), jnp.float32), 0.25, 1.75),
        "norm2_shift": scatter_about(splits[6], (CH,), 0.3, 1.75, (), jnp.float32),
        "conv2_weight": scatter_about(splits[7], (3, 3, CH, CH), (9 * CH) ** -0.5, 0.09375),
        "conv2_bias": scatter_about(splits[8], (CH,), 0.3, 1.75, (), jnp.float32),
        "out_gain": jnp.clip(1.0 + 0.15 * jax.random.normal(splits[9], (CH,), jnp.float32), 0.25, 1.75),
        "out_shift": scatter_about(splits[10], (CH,), 0.3, 1.75, (), jnp.float32),
        "out_weight": scatter_about(splits[11], (3, 3, CH, MOMENTS), (9 * CH) ** -0.5, 0.09375),
        "out_bias": scatter_about(splits[12], (MOMENTS,), 0.3, 1.75, (), jnp.float32),
        "quant_weight": scatter_about(splits[13], (MOMENTS, LATENT), MOMENTS ** -0.5, 2.0, (), jnp.float32),
        "quant_bias": scatter_about(splits[14], (LATENT,), 0.3, 1.75, (), jnp.float32),
        "time_in_weight": scatter_about(splits[15], (3, 3, 3, LATENT, TCH), (27 * LATENT) ** -0.5, 0.625),
        "time_in_bias": scatter_about(splits[16], (TCH,), 0.3, 1.75, (), jnp.float32),
        "tnorm1_gain": jnp.clip(1.0 + 0.15 * jax.random.normal(splits[17], (TCH,), jnp.float32), 0.25, 1.75),
        "tnorm1_shift": scatter_about(splits[18], (TCH,), 0.3, 1.75, (), jnp.float32),
        "time1_weight": scatter_about(splits[19], (3, 3, 3, TCH, TCH), (27 * TCH) ** -0.5, 0.109375),
        "tnorm2_gain": jnp.clip(1.0 + 0.15 * jax.random.normal(splits[20], (TCH,), jnp.float32), 0.25, 1.75),
        "tnorm2_shift": scatter_about(splits[21], (TCH,), 0.3, 1.75, (), jnp.float32),
        "time2_weight": scatter_about(splits[22], (3, 3, 3, TCH, TCH), (27 * TCH) ** -0.5, 0.109375),
        "time2_bias": scatter_about(splits[23], (TCH,), 0.3, 1.75, (), jnp.float32),
    }


EPS = 1e-06
LATENT_SCALE = 0.13025

def group_act(values, norm_gain, norm_shift):
    shape = values.shape
    grouped = values.reshape(shape[0], shape[1] * shape[2], GROUPS, shape[3] // GROUPS)
    axes = (1, 3)
    average = lax.optimization_barrier(jnp.mean(grouped, axis=axes, keepdims=True))
    centred = grouped - average
    variance = lax.optimization_barrier(jnp.mean(centred * centred, axis=axes, keepdims=True))
    scaled = (centred * lax.rsqrt(variance + EPS)).reshape(shape)
    return jax.nn.silu(scaled * norm_gain + norm_shift).astype(jnp.bfloat16)

def plane_conv(active, weight, offset):
    height, columns, channels = (active.shape[1], active.shape[2], active.shape[3])

    def one_frame(current):
        padded = jnp.pad(current, ((1, 1), (1, 1), (0, 0)))
        summed = jnp.zeros((height * columns, weight.shape[3]), jnp.float32)
        for row_off in range(3):
            for col_off in range(3):
                window = padded[row_off:row_off + height, col_off:col_off + columns].reshape(-1, channels)
                summed = summed + jnp.dot(window, weight[row_off, col_off], preferred_element_type=jnp.float32)
        return summed.reshape(height, columns, -1) + offset
    return lax.map(one_frame, active)

def clip_conv(active, weight, offset):
    count, height, columns, channels = active.shape
    padded = jnp.pad(active, ((2, 0), (1, 1), (1, 1), (0, 0)))
    summed = jnp.zeros((count * height * columns, weight.shape[4]), jnp.float32)
    for time_off in range(3):
        for row_off in range(3):
            for col_off in range(3):
                window = padded[time_off:time_off + count, row_off:row_off + height, col_off:col_off + columns]
                summed = summed + jnp.dot(window.reshape(-1, channels), weight[time_off, row_off, col_off], preferred_element_type=jnp.float32)
    return summed.reshape(count, height, columns, -1) + offset

def reference(video, norm1_gain, norm1_shift, conv1_weight, conv1_bias, norm2_gain, norm2_shift, conv2_weight, conv2_bias, out_gain, out_shift, out_weight, out_bias, quant_weight, quant_bias, time_in_weight, time_in_bias, tnorm1_gain, tnorm1_shift, time1_weight, tnorm2_gain, tnorm2_shift, time2_weight, time2_bias):
    inputs = video.astype(jnp.float32)
    first_act = group_act(inputs, norm1_gain, norm1_shift)
    hidden = plane_conv(first_act, conv1_weight, conv1_bias)
    second_act = group_act(hidden, norm2_gain, norm2_shift)
    block_out = inputs + plane_conv(second_act, conv2_weight, conv2_bias)
    head_act = group_act(block_out, out_gain, out_shift)
    moments = plane_conv(head_act, out_weight, out_bias)
    shape = moments.shape
    means = jnp.dot(moments.reshape(-1, shape[3]), quant_weight, precision=lax.Precision.HIGHEST) + quant_bias
    latent = (LATENT_SCALE * means).astype(jnp.bfloat16).reshape(shape[0], shape[1], shape[2], -1)
    lifted = clip_conv(latent, time_in_weight, time_in_bias)
    time_act = group_act(lifted, tnorm1_gain, tnorm1_shift)
    inner = clip_conv(time_act, time1_weight, 0.0)
    last_act = group_act(inner, tnorm2_gain, tnorm2_shift)
    return (lifted + clip_conv(last_act, time2_weight, time2_bias)).astype(jnp.bfloat16)
```

```python
import functools

import jax
import jax.numpy as jnp
from jax import lax
from jax.experimental import pallas as pl
from jax.experimental.pallas import tpu as pltpu
from jax.sharding import PartitionSpec as P

GROUPS = 32
EPS = 1e-06
LATENT_SCALE = 0.13025
LANES = 128
F32 = jnp.float32
BF16 = jnp.bfloat16

ANY = pl.BlockSpec(memory_space=pl.ANY)
VMEM = pl.BlockSpec(memory_space=pltpu.VMEM)
SMEM = pl.BlockSpec(memory_space=pltpu.SMEM)


def params(mib=48):
    return pltpu.CompilerParams(vmem_limit_bytes=mib * 1024 * 1024)


def lane_groups(values, size):
    lane = lax.broadcasted_iota(jnp.int32, values.shape, 1)
    step = 1
    while step < size:
        up = pltpu.roll(values, step, 1)
        down = pltpu.roll(values, LANES - step, 1)
        values = values + jnp.where((lane & step) != 0, up, down)
        step *= 2
    return values


def half_affine(parts, rows, gain, shift, count, per_group):
    total = parts[0][...]
    for part in parts[1:]:
        total = total + part[...]
    total = lane_groups(total, per_group) / count
    mean = total[0:rows]
    variance = total[rows : 2 * rows] - mean * mean
    scale = lax.rsqrt(variance + EPS) * gain
    return 0.5 * scale, 0.5 * (shift - mean * scale)


def as_row(block):
    return jnp.concatenate([block[k : k + 1, :] for k in range(block.shape[0])], axis=1)


def half_silu(values, scale, shift):
    t = values * scale + shift
    return t * jnp.tanh(t) + t


def put_sums(out_ref, first, second, rows):
    for k in range(rows):
        lanes = slice(k * LANES, (k + 1) * LANES)
        out_ref[k : k + 1, :] = first[:, lanes]
        out_ref[rows + k : rows + k + 1, :] = second[:, lanes]


def spread_columns(slots, row, at, even, odd, channels):
    half, width = even.shape
    index = lax.broadcasted_iota(jnp.int32, (half, width), 0)
    before = jnp.where(index == 0, 0.0, pltpu.roll(odd, 1, 0))
    after = jnp.where(index == half - 1, 0.0, pltpu.roll(even, half - 1, 0))
    for slot, piece in enumerate((before, even, odd, after)):
        slots[row, :, slot * channels + at : slot * channels + at + width] = piece.astype(BF16)


def input_sums_kernel(x_hbm, out_ref, xs, sems):
    lines = xs.shape[0]
    copies = [pltpu.make_async_copy(x_hbm.at[r], xs.at[r], sems.at[r]) for r in range(lines)]
    for copy in copies:
        copy.start()
    width, channels = xs.shape[1], xs.shape[2]
    first = [jnp.zeros((8, LANES), F32) for _ in range(channels // LANES)]
    second = list(first)
    for r in range(lines):
        copies[r].wait()

        def step(m, carry, r=r):
            first, second = carry
            first, second = list(first), list(second)
            at = pl.multiple_of(m * 32, 32)
            for k in range(channels // LANES):
                v = xs[r, pl.ds(at, 32), k * LANES : (k + 1) * LANES].astype(F32)
                v = v.reshape(4, 8, LANES)
                first[k] = first[k] + v.sum(0)
                second[k] = second[k] + (v * v).sum(0)
            return tuple(first), tuple(second)

        first, second = lax.fori_loop(0, width // 32, step, (tuple(first), tuple(second)))
    rows = channels // LANES
    for k in range(rows):
        out_ref[k : k + 1, :] = first[k].sum(0, keepdims=True)
        out_ref[rows + k : rows + k + 1, :] = second[k].sum(0, keepdims=True)


def input_sums(x):
    lines, width, channels = x.shape
    return pl.pallas_call(
        input_sums_kernel,
        out_shape=jax.ShapeDtypeStruct((2 * channels // LANES, LANES), F32),
        in_specs=[ANY],
        out_specs=VMEM,
        scratch_shapes=[pltpu.VMEM(x.shape, BF16), pltpu.SemaphoreType.DMA((lines,))],
        compiler_params=params(16),
        name="input_sums",
    )(x)


def conv_rows(slots, weights, bias_ref, out, sums, out_lines, own_at, own_lines, half, channels, residual):
    tile = 256
    n_tiles = channels // tile
    sums[...] = jnp.zeros_like(sums)

    def step(index, _):
        parity = index // n_tiles
        at = pl.multiple_of((index % n_tiles) * tile, tile)
        left = pl.multiple_of(parity * channels, channels)
        acc = None
        for i in range(3):
            lhs = slots[i : i + out_lines, :, pl.ds(left, 3 * channels)].reshape(out_lines * half, 3 * channels)
            part = jnp.dot(lhs, weights[i, :, pl.ds(at, tile)], preferred_element_type=F32)
            acc = part if acc is None else acc + part
        acc = acc.reshape(out_lines, half, tile) + bias_ref[:, pl.ds(at, tile)].reshape(1, 1, tile)
        if residual is not None:
            acc = acc + residual[:, parity, :, pl.ds(at, tile)].astype(F32)
        out[:, parity, :, pl.ds(at, tile)] = acc
        own = acc[own_at : own_at + own_lines].reshape(own_lines * half, tile)
        sums[0:1, pl.ds(at, tile)] += own.sum(0, keepdims=True)
        sums[1:2, pl.ds(at, tile)] += (own * own).sum(0, keepdims=True)
        return 0

    lax.fori_loop(0, 2 * n_tiles, step, 0)


def conv1_kernel(
    meta, s0, s1, s2, s3, gain, shift, bias, x_hbm, up_hbm, low_hbm, w_hbm,
    h_hbm, xp_ref, stats_ref,
    xs, rowf, slots, wv, hv, sums, sems, wsem, hsem,
    *, count, per_group, n_blocks,
):
    own = x_hbm.shape[0]
    halo = up_hbm.shape[0]
    lines, width, channels = xs.shape
    half = width // 2
    loads = [
        pltpu.make_async_copy(up_hbm, xs.at[pl.ds(0, halo)], sems.at[0]),
        pltpu.make_async_copy(x_hbm, xs.at[pl.ds(halo, own)], sems.at[1]),
        pltpu.make_async_copy(low_hbm, xs.at[pl.ds(halo + own, halo)], sems.at[2]),
    ]
    for copy in loads:
        copy.start()
    weight_load = pltpu.make_async_copy(w_hbm, wv, wsem)
    weight_load.start()
    scale, move = half_affine((s0, s1, s2, s3), channels // LANES, gain[...], shift[...], count, per_group)
    scale, move = as_row(scale), as_row(move)
    for copy in loads:
        copy.wait()
    first_line = meta[0] * own - halo

    def norm(r, _):
        line = first_line + r
        inside = (line >= 0) & (line < n_blocks * own)
        for at in range(0, channels, LANES):
            cols = slice(at, at + LANES)
            chunk = at // LANES
            rowf[chunk] = xs[r, :, cols].astype(F32)
            even = rowf[chunk, pl.ds(0, half, stride=2), :]
            odd = rowf[chunk, pl.ds(1, half, stride=2), :]
            xp_ref[r, 0, :, cols] = even.astype(BF16)
            xp_ref[r, 1, :, cols] = odd.astype(BF16)
            even = jnp.where(inside, half_silu(even, scale[:, cols], move[:, cols]), 0.0)
            odd = jnp.where(inside, half_silu(odd, scale[:, cols], move[:, cols]), 0.0)
            spread_columns(slots, r, at, even, odd, channels)
        return 0

    lax.fori_loop(0, lines, norm, 0)
    weight_load.wait()
    conv_rows(slots, wv, bias, hv, sums, lines - 2, halo - 1, own, half, channels, None)
    store = pltpu.make_async_copy(hv, h_hbm, hsem)
    store.start()
    put_sums(stats_ref, sums[0:1, :], sums[1:2, :], channels // LANES)
    store.wait()


def conv1(meta, stats, gain, shift, bias, x, up, low, weight, n_blocks):
    own, width, channels = x.shape
    halo = up.shape[0]
    lines = own + 2 * halo
    half = width // 2
    rows = channels // LANES
    count = float(n_blocks * own * width * (channels // GROUPS))
    return pl.pallas_call(
        functools.partial(conv1_kernel, count=count, per_group=channels // GROUPS, n_blocks=n_blocks),
        out_shape=(
            jax.ShapeDtypeStruct((lines - 2, 2, half, channels), F32),
            jax.ShapeDtypeStruct((lines, 2, half, channels), BF16),
            jax.ShapeDtypeStruct((2 * rows, LANES), F32),
        ),
        in_specs=[SMEM] + [VMEM] * 7 + [ANY] * 4,
        out_specs=(ANY, VMEM, VMEM),
        scratch_shapes=[
            pltpu.VMEM((lines, width, channels), BF16),
            pltpu.VMEM((channels // LANES, width, LANES), F32),
            pltpu.VMEM((lines, half, 4 * channels), BF16),
            pltpu.VMEM((3, 3 * channels, channels), BF16),
            pltpu.VMEM((lines - 2, 2, half, channels), F32),
            pltpu.VMEM((2, channels), F32),
            pltpu.SemaphoreType.DMA((3,)),
            pltpu.SemaphoreType.DMA,
            pltpu.SemaphoreType.DMA,
        ],
        compiler_params=params(48),
        name="conv1",
    )(meta, *stats, gain.reshape(rows, LANES), shift.reshape(rows, LANES), bias.reshape(1, channels), x, up, low,
      weight.reshape(3, 3 * channels, channels))


def conv2_kernel(
    meta, s0, s1, s2, s3, gain, shift, bias, h_hbm, xp_hbm, w_hbm,
    y_hbm, stats_ref,
    hs, xs, slots, wv, yv, sums, sems, xsem, wsem, ysem,
    *, count, per_group, n_blocks,
):
    lines, _, half, channels = hs.shape
    own = lines - 2
    loads = [pltpu.make_async_copy(h_hbm.at[r], hs.at[r], sems.at[r]) for r in range(lines)]
    for copy in loads:
        copy.start()
    weight_load = pltpu.make_async_copy(w_hbm, wv, wsem)
    weight_load.start()
    edge = (xp_hbm.shape[0] - own) // 2
    x_load = pltpu.make_async_copy(xp_hbm.at[pl.ds(edge, own)], xs, xsem)
    x_load.start()
    scale, move = half_affine((s0, s1, s2, s3), channels // LANES, gain[...], shift[...], count, per_group)
    scale, move = as_row(scale), as_row(move)
    for copy in loads:
        copy.wait()
    first_line = meta[0] * own - 1

    def norm(r, _):
        line = first_line + r
        inside = (line >= 0) & (line < n_blocks * own)
        for at in range(0, channels, LANES):
            cols = slice(at, at + LANES)
            even = jnp.where(inside, half_silu(hs[r, 0, :, cols], scale[:, cols], move[:, cols]), 0.0)
            odd = jnp.where(inside, half_silu(hs[r, 1, :, cols], scale[:, cols], move[:, cols]), 0.0)
            spread_columns(slots, r, at, even, odd, channels)
        return 0

    lax.fori_loop(0, lines, norm, 0)
    x_load.wait()
    weight_load.wait()
    conv_rows(slots, wv, bias, yv, sums, own, 0, own, half, channels, xs)
    store = pltpu.make_async_copy(yv, y_hbm, ysem)
    store.start()
    put_sums(stats_ref, sums[0:1, :], sums[1:2, :], channels // LANES)
    store.wait()


def conv2(meta, stats, gain, shift, bias, h, xp, weight, n_blocks):
    lines, _, half, channels = h.shape
    own = lines - 2
    rows = channels // LANES
    count = float(n_blocks * own * 2 * half * (channels // GROUPS))
    return pl.pallas_call(
        functools.partial(conv2_kernel, count=count, per_group=channels // GROUPS, n_blocks=n_blocks),
        out_shape=(
            jax.ShapeDtypeStruct((own, 2, half, channels), F32),
            jax.ShapeDtypeStruct((2 * rows, LANES), F32),
        ),
        in_specs=[SMEM] + [VMEM] * 7 + [ANY] * 3,
        out_specs=(ANY, VMEM),
        scratch_shapes=[
            pltpu.VMEM((lines, 2, half, channels), F32),
            pltpu.VMEM((own, 2, half, channels), BF16),
            pltpu.VMEM((lines, half, 4 * channels), BF16),
            pltpu.VMEM((3, 3 * channels, channels), BF16),
            pltpu.VMEM((own, 2, half, channels), F32),
            pltpu.VMEM((2, channels), F32),
            pltpu.SemaphoreType.DMA((lines,)),
            pltpu.SemaphoreType.DMA,
            pltpu.SemaphoreType.DMA,
            pltpu.SemaphoreType.DMA,
        ],
        compiler_params=params(48),
        name="conv2",
    )(meta, *stats, gain.reshape(rows, LANES), shift.reshape(rows, LANES), bias.reshape(1, channels), h, xp,
      weight.reshape(3, 3 * channels, channels))


def column_shift(values, tap, half):
    size = values.shape[1]
    lane = lax.broadcasted_iota(jnp.int32, values.shape, 1) % (2 * half)
    even = lane < half
    if tap == 0:
        moved = jnp.where(even, pltpu.roll(values, size - (half - 1), 1), pltpu.roll(values, half, 1))
        return jnp.where(lane == 0, 0.0, moved)
    moved = jnp.where(even, pltpu.roll(values, size - half, 1), pltpu.roll(values, half - 1, 1))
    return jnp.where(lane == 2 * half - 1, 0.0, moved)


def head_kernel(
    meta, s0, s1, s2, s3, gain, shift, w_ref, q_ref, b_ref, y_hbm, part_ref, up_ref, low_ref, ys, act, sems,
    *, count, per_group, n_blocks, n_send,
):
    own, _, half, channels = ys.shape
    width = 2 * half
    loads = [pltpu.make_async_copy(y_hbm.at[r], ys.at[r], sems.at[r]) for r in range(own)]
    for copy in loads:
        copy.start()
    scale, move = half_affine((s0, s1, s2, s3), channels // LANES, gain[...], shift[...], count, per_group)
    scale, move = as_row(scale), as_row(move)
    for copy in loads:
        copy.wait()

    def norm(r, _):
        for parity in range(2):
            for at in range(0, channels, LANES):
                cols = slice(at, at + LANES)
                act[r, parity, :, cols] = half_silu(ys[r, parity, :, cols], scale[:, cols], move[:, cols]).astype(BF16)
        return 0

    lax.fori_loop(0, own, norm, 0)
    flat = act[...].reshape(own * width, channels)
    taps = lax.dot_general(w_ref[...], flat, (((1,), (1,)), ((), ())), preferred_element_type=F32)
    size = part_ref.shape[1]
    moments_n = taps.shape[0] // 9
    spare = jnp.zeros((moments_n, size - own * width), F32)
    total = None
    for i in range(3):
        piece = None
        for j in range(3):
            at = (3 * i + j) * moments_n
            one = taps[at : at + moments_n]
            one = one if j == 1 else column_shift(one, j, half)
            piece = one if piece is None else piece + one
        piece = jnp.concatenate([piece, spare], axis=1)
        if i < 2:
            piece = pltpu.roll(piece, (2 - i) * width, 1)
        total = piece if total is None else total + piece
    lane = lax.broadcasted_iota(jnp.int32, (1, size), 1)
    own_lane = (lane >= width) & (lane < (own + 1) * width)
    latents = []
    for c in range(q_ref.shape[1]):
        value = LATENT_SCALE * jnp.sum(total * q_ref[:, c : c + 1], axis=0, keepdims=True)
        latents.append(value + jnp.where(own_lane, b_ref[c : c + 1, 0:1], 0.0))
    latent = jnp.concatenate(latents, axis=0)
    keep = ((lane >= width) | (meta[0] > 0)) & ((lane < (own + 1) * width) | (meta[0] < n_blocks - 1))
    part_ref[...] = jnp.where(keep, latent, 0.0)
    up_ref[...] = latent[:, : n_send * width]
    low_ref[...] = pltpu.roll(latent, size - (own + 2 - n_send) * width, 1)[:, : n_send * width]


def head(meta, stats, gain, shift, y, weight, bias, quant_weight, quant_bias, n_blocks, n_send):
    own, _, half, channels = y.shape
    width = 2 * half
    rows = channels // LANES
    moments, latents = quant_weight.shape
    count = float(n_blocks * own * width * (channels // GROUPS))
    size = -(-((own + 2) * width) // LANES) * LANES
    taps = weight.transpose(0, 1, 3, 2).reshape(9 * moments, channels)
    offset = LATENT_SCALE * (jnp.sum(bias[:, None] * quant_weight, axis=0) + quant_bias)
    offset = jnp.broadcast_to(offset[:, None], (latents, LANES))
    return pl.pallas_call(
        functools.partial(head_kernel, count=count, per_group=channels // GROUPS, n_blocks=n_blocks, n_send=n_send),
        out_shape=(
            jax.ShapeDtypeStruct((latents, size), F32),
            jax.ShapeDtypeStruct((latents, n_send * width), F32),
            jax.ShapeDtypeStruct((latents, n_send * width), F32),
        ),
        in_specs=[SMEM] + [VMEM] * 9 + [ANY],
        out_specs=(VMEM, VMEM, VMEM),
        scratch_shapes=[
            pltpu.VMEM((own, 2, half, channels), F32),
            pltpu.VMEM((own, 2, half, channels), BF16),
            pltpu.SemaphoreType.DMA((own,)),
        ],
        compiler_params=params(32),
        name="head",
    )(meta, *stats, gain.reshape(rows, LANES), shift.reshape(rows, LANES), taps, quant_weight, offset, y)


def lift_kernel(meta, w_ref, bias_ref, *refs, own, half, n_frames, n_out):
    latents = refs[:n_frames]
    t0_hbm, stats_ref, stack, patches, t0v, sem = refs[n_frames:]
    width = 2 * half
    out_lines = own + 4
    pixels = out_lines * width
    depth, size = stack.shape
    each = latents[0].shape[0]
    for k in range(n_frames):
        value = latents[k][...].astype(F32)
        stack[k * each : (k + 1) * each, :] = jnp.where(meta[1] >= k, value, 0.0)
    frames = stack[...]
    patches[...] = jnp.zeros_like(patches)
    for j in range(3):
        moved = frames if j == 1 else column_shift(frames, j, half)
        for i in range(3):
            piece = moved if i == 0 else pltpu.roll(moved, size - i * width, 1)
            at = (3 * i + j) * depth
            patches[at : at + depth, :] = piece[:, :pixels]
    lhs = jnp.transpose(patches[...], (1, 0)).astype(BF16)
    channels = bias_ref.shape[1]
    for g in range(n_out):
        cols = slice(g * channels, (g + 1) * channels)
        value = jnp.dot(lhs, w_ref[:, cols], preferred_element_type=F32) + bias_ref[...]
        t0v[:, cols] = value
        mine = value[2 * width : (2 + own) * width]
        stats_ref[g : g + 1, :] = mine.sum(0, keepdims=True)
        stats_ref[n_out + g : n_out + g + 1, :] = (mine * mine).sum(0, keepdims=True)
    store = pltpu.make_async_copy(t0v, t0_hbm, sem)
    store.start()
    store.wait()


def lift_weights(weight, n_frames, n_out):
    _, _, _, latents, channels = weight.shape
    back = weight[::-1].transpose(1, 2, 0, 3, 4).reshape(9, 3 * latents, channels)
    blocks = []
    for g in range(n_out):
        blocks.append(jnp.pad(back, ((0, 0), (g * latents, (n_frames - 3 - g) * latents), (0, 0))))
    whole = jnp.concatenate(blocks, axis=2).reshape(9 * n_frames * latents, n_out * channels)
    extra = -whole.shape[0] % 256
    return jnp.pad(whole, ((0, extra), (0, 0)))


def lift(meta, packed, bias, latents, own, half, n_out):
    n_frames = len(latents)
    each, size = latents[0].shape
    channels = bias.shape[0]
    pixels = (own + 4) * 2 * half
    stat_rows = -(-2 * n_out // 8) * 8
    return pl.pallas_call(
        functools.partial(lift_kernel, own=own, half=half, n_frames=n_frames, n_out=n_out),
        out_shape=(
            jax.ShapeDtypeStruct((pixels, n_out * channels), F32),
            jax.ShapeDtypeStruct((stat_rows, channels), F32),
        ),
        in_specs=[SMEM] + [VMEM] * (2 + n_frames),
        out_specs=(ANY, VMEM),
        scratch_shapes=[
            pltpu.VMEM((n_frames * each, size), F32),
            pltpu.VMEM((packed.shape[0], pixels), F32),
            pltpu.VMEM((pixels, n_out * channels), F32),
            pltpu.SemaphoreType.DMA,
        ],
        compiler_params=params(32),
        name="lift",
    )(meta, packed, bias.reshape(1, channels), *latents)


def pair_weight_copies(w_hbm, wv, sems, channels):
    copies = []
    for c in range(2):
        for j in range(3):
            target = wv.at[:, pl.ds((j + c) * channels, channels), pl.ds(c * channels, channels)]
            copies.append(pltpu.make_async_copy(w_hbm.at[:, j], target, sems.at[3 * c + j]))
    return copies


def clear_pair_weights(wv, channels):
    zero = jnp.zeros((wv.shape[0], channels, channels), BF16)
    wv[:, 3 * channels : 4 * channels, 0:channels] = zero
    wv[:, 0:channels, channels : 2 * channels] = zero


def time1_kernel(
    meta, s0, s1, s2, s3, gain, shift, t0_hbm, w_hbm, t1_hbm, stats_ref,
    ts, slots, wv, t1v, sem, wsems, osem,
    *, count, per_group, n_blocks, own, n_out,
):
    frames, lines, half, _ = slots.shape
    channels = gain.shape[1]
    width = 2 * half
    load = pltpu.make_async_copy(t0_hbm, ts, sem)
    load.start()
    weight_loads = pair_weight_copies(w_hbm, wv, wsems, channels)
    for copy in weight_loads:
        copy.start()
    clear_pair_weights(wv, channels)
    scale, move = half_affine((s0, s1, s2, s3), frames, gain[...], shift[...], count, per_group)
    load.wait()
    first_line = meta[0] * own - 2
    for k in range(frames):
        cols = slice(k * channels, (k + 1) * channels)

        def norm(r, _, k=k, cols=cols):
            line = first_line + r
            inside = (line >= 0) & (line < n_blocks * own) & (meta[1] >= k)
            at = pl.multiple_of(r * width, width)
            even = half_silu(ts[pl.ds(at, half), cols], scale[k : k + 1], move[k : k + 1])
            odd = half_silu(ts[pl.ds(at + half, half), cols], scale[k : k + 1], move[k : k + 1])
            even = jnp.where(inside, even, 0.0)
            odd = jnp.where(inside, odd, 0.0)
            spread_columns(slots.at[k], r, 0, even, odd, channels)
            return 0

        lax.fori_loop(0, lines, norm, 0)
    for copy in weight_loads:
        copy.wait()
    out_lines = lines - 2
    for k in range(n_out):
        acc = None
        for t in range(3):
            for i in range(3):
                lhs = slots[k + 2 - t, i : i + out_lines].reshape(out_lines * half, 4 * channels)
                part = jnp.dot(lhs, wv[3 * t + i], preferred_element_type=F32)
                acc = part if acc is None else acc + part
        t1v[k] = acc.reshape(out_lines, half, 2 * channels)
        mine = acc[half : (1 + own) * half]
        first = mine.sum(0, keepdims=True)
        second = (mine * mine).sum(0, keepdims=True)
        stats_ref[k : k + 1, :] = first[:, :channels] + first[:, channels:]
        stats_ref[n_out + k : n_out + k + 1, :] = second[:, :channels] + second[:, channels:]
    store = pltpu.make_async_copy(t1v, t1_hbm, osem)
    store.start()
    store.wait()


def time1(meta, stats, gain, shift, t0, weight, n_blocks, own, half, n_frames, n_out):
    channels = gain.shape[0]
    count = float(n_blocks * own * 2 * half * (channels // GROUPS))
    lines = own + 4
    return pl.pallas_call(
        functools.partial(
            time1_kernel, count=count, per_group=channels // GROUPS, n_blocks=n_blocks, own=own, n_out=n_out
        ),
        out_shape=(
            jax.ShapeDtypeStruct((n_out, lines - 2, half, 2 * channels), F32),
            jax.ShapeDtypeStruct((-(-2 * n_out // 8) * 8, channels), F32),
        ),
        in_specs=[SMEM] + [VMEM] * 6 + [ANY] * 2,
        out_specs=(ANY, VMEM),
        scratch_shapes=[
            pltpu.VMEM(t0.shape, F32),
            pltpu.VMEM((n_frames, lines, half, 4 * channels), BF16),
            pltpu.VMEM((9, 4 * channels, 2 * channels), BF16),
            pltpu.VMEM((n_out, lines - 2, half, 2 * channels), F32),
            pltpu.SemaphoreType.DMA,
            pltpu.SemaphoreType.DMA((6,)),
            pltpu.SemaphoreType.DMA,
        ],
        compiler_params=params(48),
        name="time1",
    )(meta, *stats, gain.reshape(1, channels), shift.reshape(1, channels), t0,
      weight.reshape(9, 3, channels, channels))


def time2_kernel(
    meta, s0, s1, s2, s3, gain, shift, bias, t1_hbm, t0_hbm, w_hbm, out_hbm,
    ts, t0s, slots, wv, rowf, outv, sem, t0sem, wsems, osem,
    *, count, per_group, n_blocks,
):
    frames, lines, half, _ = slots.shape
    own = lines - 2
    channels = gain.shape[1]
    width = 2 * half
    load = pltpu.make_async_copy(t1_hbm, ts, sem)
    load.start()
    weight_loads = pair_weight_copies(w_hbm, wv, wsems, channels)
    for copy in weight_loads:
        copy.start()
    t0_load = pltpu.make_async_copy(t0_hbm.at[pl.ds(2 * width, own * width), pl.ds(0, channels)], t0s, t0sem)
    t0_load.start()
    clear_pair_weights(wv, channels)
    scale, move = half_affine((s0, s1, s2, s3), frames, gain[...], shift[...], count, per_group)
    load.wait()
    first_line = meta[0] * own - 1
    for k in range(frames):

        def norm(r, _, k=k):
            line = first_line + r
            inside = (line >= 0) & (line < n_blocks * own) & (meta[1] >= k)
            even = half_silu(ts[k, r, :, 0:channels], scale[k : k + 1], move[k : k + 1])
            odd = half_silu(ts[k, r, :, channels : 2 * channels], scale[k : k + 1], move[k : k + 1])
            even = jnp.where(inside, even, 0.0)
            odd = jnp.where(inside, odd, 0.0)
            spread_columns(slots.at[k], r, 0, even, odd, channels)
            return 0

        lax.fori_loop(0, lines, norm, 0)
    for copy in weight_loads:
        copy.wait()
    acc = None
    for t in range(3):
        for i in range(3):
            lhs = slots[2 - t, i : i + own].reshape(own * half, 4 * channels)
            part = jnp.dot(lhs, wv[3 * t + i], preferred_element_type=F32)
            acc = part if acc is None else acc + part
    acc = acc.reshape(own, half, 2 * channels)
    t0_load.wait()
    for r in range(own):
        for parity in range(2):
            at = r * width + parity * half
            value = acc[r, :, parity * channels : (parity + 1) * channels] + bias[...] + t0s[at : at + half, :]
            rowf[r, pl.ds(parity, half, stride=2), :] = value
        outv[r] = rowf[r].astype(BF16)
    store = pltpu.make_async_copy(outv, out_hbm.at[0], osem)
    store.start()
    store.wait()


def time2(meta, stats, gain, shift, bias, t1, t0, weight, n_blocks):
    frames, lines, half, _ = t1.shape
    own = lines - 2
    channels = gain.shape[0]
    count = float(n_blocks * own * 2 * half * (channels // GROUPS))
    return pl.pallas_call(
        functools.partial(time2_kernel, count=count, per_group=channels // GROUPS, n_blocks=n_blocks),
        out_shape=jax.ShapeDtypeStruct((1, own, 2 * half, channels), BF16),
        in_specs=[SMEM] + [VMEM] * 7 + [ANY] * 3,
        out_specs=ANY,
        scratch_shapes=[
            pltpu.VMEM(t1.shape, F32),
            pltpu.VMEM((own * 2 * half, channels), F32),
            pltpu.VMEM((frames, lines, half, 4 * channels), BF16),
            pltpu.VMEM((9, 4 * channels, 2 * channels), BF16),
            pltpu.VMEM((own, 2 * half, channels), F32),
            pltpu.VMEM((own, 2 * half, channels), BF16),
            pltpu.SemaphoreType.DMA,
            pltpu.SemaphoreType.DMA,
            pltpu.SemaphoreType.DMA((6,)),
            pltpu.SemaphoreType.DMA,
        ],
        compiler_params=params(48),
        name="time2",
    )(meta, *stats, gain.reshape(1, channels), shift.reshape(1, channels), bias.reshape(1, channels), t1, t0,
      weight.reshape(9, 3, channels, channels))


def turned(block, axis, distance):
    count = lax.axis_size(axis)
    return lax.ppermute(block, axis, [(i, (i + distance) % count) for i in range(count)])


def from_all(block):
    return [block] + [turned(block, "rows", d) for d in range(1, lax.axis_size("rows"))]


def body(
    video, norm1_gain, norm1_shift, conv1_weight, conv1_bias, norm2_gain, norm2_shift, conv2_weight, conv2_bias,
    out_gain, out_shift, out_weight, out_bias, quant_weight, quant_bias, time_in_weight, time_in_bias,
    tnorm1_gain, tnorm1_shift, time1_weight, tnorm2_gain, tnorm2_shift, time2_weight, time2_bias,
):
    x = video[0]
    own, width, _ = x.shape
    half = width // 2
    n_blocks = lax.axis_size("rows")
    meta = jnp.stack([lax.axis_index("rows"), lax.axis_index("frames")]).astype(jnp.int32)
    up = turned(x[own - 2 :], "rows", 1)
    low = turned(x[:2], "rows", -1)
    stats = from_all(input_sums(x))
    h, xp, sums = conv1(meta, stats, norm1_gain, norm1_shift, conv1_bias, x, up, low, conv1_weight, n_blocks)
    y, sums = conv2(meta, from_all(sums), norm2_gain, norm2_shift, conv2_bias, h, xp, conv2_weight, n_blocks)
    part, to_up, to_low = head(
        meta, from_all(sums), out_gain, out_shift, y, out_weight, out_bias, quant_weight, quant_bias, n_blocks, 4
    )
    above = turned(to_low, "rows", 1)
    below = turned(to_up, "rows", -1)
    size = -(-((own + 6) * width) // LANES) * LANES
    row = lax.axis_index("rows")
    above = jnp.where(row > 0, above, 0.0)
    below = jnp.where(row < n_blocks - 1, below, 0.0)
    latent = (
        jnp.pad(part, ((0, 0), (2 * width, size))) [:, :size]
        + jnp.pad(above, ((0, 0), (0, size - 4 * width)))
        + jnp.pad(below, ((0, 0), ((own + 2) * width, size - (own + 6) * width)))
    ).astype(BF16)
    near = jnp.concatenate([latent, turned(latent, "frames", 1), turned(latent, "frames", 2)], axis=0)
    far = turned(near, "frames", 3)
    farther = turned(near, "frames", 4)
    each = latent.shape[0]
    latents = [near[k * each : (k + 1) * each] for k in range(3)] + [far[k * each : (k + 1) * each] for k in range(3)]
    latents.append(farther[2 * each : 3 * each])
    t0, sums = lift(meta, lift_weights(time_in_weight, 7, 5), time_in_bias, latents, own, half, 5)
    t1, sums = time1(meta, from_all(sums), tnorm1_gain, tnorm1_shift, t0, time1_weight, n_blocks, own, half, 5, 3)
    return time2(meta, from_all(sums), tnorm2_gain, tnorm2_shift, time2_bias, t1, t0, time2_weight, n_blocks)


def solution(mesh):
    return jax.shard_map(
        body,
        mesh=mesh,
        in_specs=(P("frames", "rows", None, None),) + (P(),) * 23,
        out_specs=P("frames", "rows", None, None),
        check_vma=False,
    )
```

```python
import functools

import jax
import jax.numpy as jnp
from jax import lax
from jax.experimental import pallas as pl
from jax.experimental.pallas import tpu as pltpu
from jax.sharding import PartitionSpec as P

GROUPS = 32
EPS = 1e-06
LATENT_SCALE = 0.13025
LANES = 128
F32 = jnp.float32
BF16 = jnp.bfloat16

HBM = pl.BlockSpec(memory_space=pltpu.HBM)
VMEM = pl.BlockSpec(memory_space=pltpu.VMEM)
SMEM = pl.BlockSpec(memory_space=pltpu.SMEM)


def in_hbm(array):
    return pltpu.with_memory_space_constraint(array, pltpu.HBM)


def params(mib=48):
    return pltpu.CompilerParams(vmem_limit_bytes=mib * 1024 * 1024)


def cost(flops):
    return pl.CostEstimate(flops=int(flops), transcendentals=0, bytes_accessed=0)


def lane_groups(values, size):
    lane = lax.broadcasted_iota(jnp.int32, values.shape, 1)
    step = 1
    while step < size:
        up = pltpu.roll(values, step, 1)
        down = pltpu.roll(values, LANES - step, 1)
        values = values + jnp.where((lane & step) != 0, up, down)
        step *= 2
    return values


def half_affine(parts, rows, gain, shift, count, per_group):
    total = parts[0][...]
    for part in parts[1:]:
        total = total + part[...]
    total = lane_groups(total, per_group) / count
    mean = total[0:rows]
    variance = total[rows : 2 * rows] - mean * mean
    scale = lax.rsqrt(variance + EPS) * gain
    return 0.5 * scale, 0.5 * (shift - mean * scale)


def as_row(block):
    return jnp.concatenate([block[k : k + 1, :] for k in range(block.shape[0])], axis=1)


def half_silu(values, scale, shift):
    t = values * scale + shift
    return t * jnp.tanh(t) + t


def put_sums(out_ref, first, second, rows):
    for k in range(rows):
        lanes = slice(k * LANES, (k + 1) * LANES)
        out_ref[k : k + 1, :] = first[:, lanes]
        out_ref[rows + k : rows + k + 1, :] = second[:, lanes]


def spread_columns(slots, row, at, even, odd, channels):
    half, width = even.shape
    index = lax.broadcasted_iota(jnp.int32, (half, width), 0)
    before = jnp.where(index == 0, 0.0, pltpu.roll(odd, 1, 0))
    after = jnp.where(index == half - 1, 0.0, pltpu.roll(even, half - 1, 0))
    for slot, piece in enumerate((before, even, odd, after)):
        slots[row, :, slot * channels + at : slot * channels + at + width] = piece.astype(BF16)


def input_sums_kernel(x_ref, out_ref):
    lines, width, channels = x_ref.shape
    rows = channels // LANES

    def step(r, carry):
        first, second = list(carry[0]), list(carry[1])
        for k in range(rows):
            v = x_ref[r, :, k * LANES : (k + 1) * LANES].astype(F32).reshape(width // 8, 8, LANES)
            first[k] = first[k] + v.sum(0)
            second[k] = second[k] + (v * v).sum(0)
        return tuple(first), tuple(second)

    zero = tuple(jnp.zeros((8, LANES), F32) for _ in range(rows))
    first, second = lax.fori_loop(0, lines, step, (zero, zero))
    for k in range(rows):
        out_ref[k : k + 1, :] = first[k].sum(0, keepdims=True)
        out_ref[rows + k : rows + k + 1, :] = second[k].sum(0, keepdims=True)


def input_sums(x):
    channels = x.shape[2]
    return pl.pallas_call(
        input_sums_kernel,
        out_shape=jax.ShapeDtypeStruct((2 * channels // LANES, LANES), F32),
        in_specs=[VMEM],
        out_specs=VMEM,
        compiler_params=params(6),
        cost_estimate=cost(6e9),
        name="input_sums",
    )(x)


def conv_rows(slots, weights, bias_ref, out, sums, out_lines, own_at, own_lines, half, channels, residual):
    tile = 256
    n_tiles = channels // tile
    sums[...] = jnp.zeros_like(sums)

    def step(index, _):
        parity = index // n_tiles
        at = pl.multiple_of((index % n_tiles) * tile, tile)
        left = pl.multiple_of(parity * channels, channels)
        acc = None
        for i in range(3):
            lhs = slots[i : i + out_lines, :, pl.ds(left, 3 * channels)].reshape(out_lines * half, 3 * channels)
            part = jnp.dot(lhs, weights[i, :, pl.ds(at, tile)], preferred_element_type=F32)
            acc = part if acc is None else acc + part
        acc = acc.reshape(out_lines, half, tile) + bias_ref[:, pl.ds(at, tile)].reshape(1, 1, tile)
        if residual is not None:
            acc = acc + residual[:, parity, :, pl.ds(at, tile)].astype(F32)
        out[:, parity, :, pl.ds(at, tile)] = acc
        own = acc[own_at : own_at + own_lines].reshape(own_lines * half, tile)
        sums[0:1, pl.ds(at, tile)] += own.sum(0, keepdims=True)
        sums[1:2, pl.ds(at, tile)] += (own * own).sum(0, keepdims=True)
        return 0

    lax.fori_loop(0, 2 * n_tiles, step, 0)


def conv1_kernel(
    meta, s0, s1, s2, s3, gain, shift, bias, x_ref, up_ref, low_ref, w_hbm,
    h_ref, xp_ref, stats_ref,
    rowf, slots, wv, sums, wsem,
    *, count, per_group, n_blocks,
):
    own, width, channels = x_ref.shape
    halo = up_ref.shape[0]
    lines = own + 2 * halo
    half = width // 2
    weight_load = pltpu.make_async_copy(w_hbm, wv, wsem)
    weight_load.start()
    scale, move = half_affine((s0, s1, s2, s3), channels // LANES, gain[...], shift[...], count, per_group)
    scale, move = as_row(scale), as_row(move)
    first_line = meta[0] * own - halo

    def norm(source, at_line, r, keep):
        line = first_line + at_line + r
        inside = (line >= 0) & (line < n_blocks * own)
        for at in range(0, channels, LANES):
            cols = slice(at, at + LANES)
            chunk = at // LANES
            rowf[chunk] = source[r, :, cols].astype(F32)
            even = rowf[chunk, pl.ds(0, half, stride=2), :]
            odd = rowf[chunk, pl.ds(1, half, stride=2), :]
            if keep:
                xp_ref[r, 0, :, cols] = even.astype(BF16)
                xp_ref[r, 1, :, cols] = odd.astype(BF16)
            even = jnp.where(inside, half_silu(even, scale[:, cols], move[:, cols]), 0.0)
            odd = jnp.where(inside, half_silu(odd, scale[:, cols], move[:, cols]), 0.0)
            spread_columns(slots, at_line + r, at, even, odd, channels)

    pl.loop(0, halo)(lambda r: norm(up_ref, 0, r, False))
    pl.loop(0, own)(lambda r: norm(x_ref, halo, r, True))
    pl.loop(0, halo)(lambda r: norm(low_ref, halo + own, r, False))
    weight_load.wait()
    conv_rows(slots, wv, bias, h_ref, sums, lines - 2, halo - 1, own, half, channels, None)
    put_sums(stats_ref, sums[0:1, :], sums[1:2, :], channels // LANES)


def conv1(meta, stats, gain, shift, bias, x, up, low, weight, n_blocks):
    own, width, channels = x.shape
    halo = up.shape[0]
    lines = own + 2 * halo
    half = width // 2
    rows = channels // LANES
    count = float(n_blocks * own * width * (channels // GROUPS))
    return pl.pallas_call(
        functools.partial(conv1_kernel, count=count, per_group=channels // GROUPS, n_blocks=n_blocks),
        out_shape=(
            pltpu.VMEM((lines - 2, 2, half, channels), F32),
            pltpu.VMEM((own, 2, half, channels), BF16),
            jax.ShapeDtypeStruct((2 * rows, LANES), F32),
        ),
        in_specs=[SMEM] + [VMEM] * 10 + [HBM],
        out_specs=(VMEM, VMEM, VMEM),
        scratch_shapes=[
            pltpu.VMEM((channels // LANES, width, LANES), F32),
            pltpu.VMEM((lines, half, 4 * channels), BF16),
            pltpu.VMEM((3, 3 * channels, channels), BF16),
            pltpu.VMEM((2, channels), F32),
            pltpu.SemaphoreType.DMA,
        ],
        compiler_params=params(26),
        cost_estimate=cost(40e9),
        name="conv1",
    )(meta, *stats, gain.reshape(rows, LANES), shift.reshape(rows, LANES), bias.reshape(1, channels), x, up, low,
      in_hbm(weight.reshape(3, 3 * channels, channels)))


def conv2_kernel(
    meta, s0, s1, s2, s3, gain, shift, bias, hs, xs, w_hbm,
    y_ref, stats_ref,
    slots, wv, sums, wsem,
    *, count, per_group, n_blocks,
):
    lines, _, half, channels = hs.shape
    own = lines - 2
    weight_load = pltpu.make_async_copy(w_hbm, wv, wsem)
    weight_load.start()
    scale, move = half_affine((s0, s1, s2, s3), channels // LANES, gain[...], shift[...], count, per_group)
    scale, move = as_row(scale), as_row(move)
    first_line = meta[0] * own - 1

    def norm(r, _):
        line = first_line + r
        inside = (line >= 0) & (line < n_blocks * own)
        for at in range(0, channels, LANES):
            cols = slice(at, at + LANES)
            even = jnp.where(inside, half_silu(hs[r, 0, :, cols], scale[:, cols], move[:, cols]), 0.0)
            odd = jnp.where(inside, half_silu(hs[r, 1, :, cols], scale[:, cols], move[:, cols]), 0.0)
            spread_columns(slots, r, at, even, odd, channels)
        return 0

    lax.fori_loop(0, lines, norm, 0)
    weight_load.wait()
    conv_rows(slots, wv, bias, y_ref, sums, own, 0, own, half, channels, xs)
    put_sums(stats_ref, sums[0:1, :], sums[1:2, :], channels // LANES)


def conv2(meta, stats, gain, shift, bias, h, xp, weight, n_blocks):
    lines, _, half, channels = h.shape
    own = lines - 2
    rows = channels // LANES
    count = float(n_blocks * own * 2 * half * (channels // GROUPS))
    return pl.pallas_call(
        functools.partial(conv2_kernel, count=count, per_group=channels // GROUPS, n_blocks=n_blocks),
        out_shape=(
            pltpu.VMEM((own, 2, half, channels), F32),
            jax.ShapeDtypeStruct((2 * rows, LANES), F32),
        ),
        in_specs=[SMEM] + [VMEM] * 9 + [HBM],
        out_specs=(VMEM, VMEM),
        scratch_shapes=[
            pltpu.VMEM((lines, half, 4 * channels), BF16),
            pltpu.VMEM((3, 3 * channels, channels), BF16),
            pltpu.VMEM((2, channels), F32),
            pltpu.SemaphoreType.DMA,
        ],
        compiler_params=params(26),
        cost_estimate=cost(30e9),
        name="conv2",
    )(meta, *stats, gain.reshape(rows, LANES), shift.reshape(rows, LANES), bias.reshape(1, channels), h, xp,
      in_hbm(weight.reshape(3, 3 * channels, channels)))


def column_shift(values, tap, half):
    size = values.shape[1]
    lane = lax.broadcasted_iota(jnp.int32, values.shape, 1) % (2 * half)
    even = lane < half
    if tap == 0:
        moved = jnp.where(even, pltpu.roll(values, size - (half - 1), 1), pltpu.roll(values, half, 1))
        return jnp.where(lane == 0, 0.0, moved)
    moved = jnp.where(even, pltpu.roll(values, size - half, 1), pltpu.roll(values, half - 1, 1))
    return jnp.where(lane == 2 * half - 1, 0.0, moved)


def head_kernel(
    meta, s0, s1, s2, s3, gain, shift, w_ref, b_ref, q_ref, qb_ref, ys, part_ref, up_ref, low_ref, act,
    *, count, per_group, n_blocks, n_send,
):
    own, _, half, channels = ys.shape
    width = 2 * half
    scale, move = half_affine((s0, s1, s2, s3), channels // LANES, gain[...], shift[...], count, per_group)
    scale, move = as_row(scale), as_row(move)

    def norm(r, _):
        for parity in range(2):
            for at in range(0, channels, LANES):
                cols = slice(at, at + LANES)
                act[r, parity, :, cols] = half_silu(ys[r, parity, :, cols], scale[:, cols], move[:, cols]).astype(BF16)
        return 0

    lax.fori_loop(0, own, norm, 0)
    flat = act[...].reshape(own * width, channels)
    taps = lax.dot_general(w_ref[...], flat, (((1,), (1,)), ((), ())), preferred_element_type=F32)
    size = part_ref.shape[1]
    moments_n = taps.shape[0] // 9
    spare = jnp.zeros((moments_n, size - own * width), F32)
    total = None
    for i in range(3):
        piece = None
        for j in range(3):
            at = (3 * i + j) * moments_n
            one = taps[at : at + moments_n]
            one = one if j == 1 else column_shift(one, j, half)
            piece = one if piece is None else piece + one
        piece = jnp.concatenate([piece, spare], axis=1)
        if i < 2:
            piece = pltpu.roll(piece, (2 - i) * width, 1)
        total = piece if total is None else total + piece
    lane = lax.broadcasted_iota(jnp.int32, (1, size), 1)
    own_lane = (lane >= width) & (lane < (own + 1) * width)
    latents = []
    for c in range(q_ref.shape[0]):
        value, offset = None, qb_ref[c]
        for o in range(moments_n):
            term = total[o : o + 1, :] * q_ref[c, o]
            value = term if value is None else value + term
            offset = offset + b_ref[o] * q_ref[c, o]
        latents.append(LATENT_SCALE * (value + jnp.where(own_lane, offset, 0.0)))
    latent = jnp.concatenate(latents, axis=0)
    keep = ((lane >= width) | (meta[0] > 0)) & ((lane < (own + 1) * width) | (meta[0] < n_blocks - 1))
    part_ref[...] = jnp.where(keep, latent, 0.0)
    up_ref[...] = latent[:, : n_send * width]
    low_ref[...] = pltpu.roll(latent, size - (own + 2 - n_send) * width, 1)[:, : n_send * width]


def head(meta, stats, gain, shift, y, weight, bias, quant_weight, quant_bias, n_blocks, n_send):
    own, _, half, channels = y.shape
    width = 2 * half
    rows = channels // LANES
    moments, latents = quant_weight.shape
    count = float(n_blocks * own * width * (channels // GROUPS))
    size = -(-((own + 2) * width) // LANES) * LANES
    taps = weight.transpose(0, 1, 3, 2).reshape(9 * moments, channels)
    return pl.pallas_call(
        functools.partial(head_kernel, count=count, per_group=channels // GROUPS, n_blocks=n_blocks, n_send=n_send),
        out_shape=(
            jax.ShapeDtypeStruct((latents, size), F32),
            jax.ShapeDtypeStruct((latents, n_send * width), F32),
            jax.ShapeDtypeStruct((latents, n_send * width), F32),
        ),
        in_specs=[SMEM] + [VMEM] * 7 + [SMEM] * 3 + [VMEM],
        out_specs=(VMEM, VMEM, VMEM),
        scratch_shapes=[pltpu.VMEM((own, 2, half, channels), BF16)],
        compiler_params=params(12),
        cost_estimate=cost(10e9),
        name="head",
    )(meta, *stats, gain.reshape(rows, LANES), shift.reshape(rows, LANES), taps, bias, quant_weight.T, quant_bias, y)


def lift_kernel(meta, w_ref, bias_ref, latents, t0_ref, stats_ref, stack, patches, weights, *, own, half, n_frames, n_out):
    width = 2 * half
    out_lines = own + 4
    pixels = out_lines * width
    depth, size = stack.shape
    each = latents.shape[1]
    channels = bias_ref.shape[1]
    for s in range(n_frames):
        frame = meta[1] - (n_frames - 1 - s)
        value = latents[jnp.maximum(frame, 0)].astype(F32)
        stack[s * each : (s + 1) * each, :] = jnp.where(frame >= 0, value, 0.0)
    frames = stack[...]
    patches[9 * depth :, :] = jnp.zeros_like(patches[9 * depth :, :])
    weights[...] = jnp.zeros_like(weights)
    for j in range(3):
        moved = frames if j == 1 else column_shift(frames, j, half)
        for i in range(3):
            piece = moved if i == 0 else pltpu.roll(moved, size - i * width, 1)
            at = (3 * i + j) * depth
            patches[at : at + depth, :] = piece[:, :pixels]
            for t in range(3):
                tap = w_ref[9 * t + 3 * i + j].astype(F32)
                for g in range(n_out):
                    row = at + (n_frames - 3 - g + t) * each
                    weights[row : row + each, g * channels : (g + 1) * channels] = tap
    lhs = jnp.transpose(patches[...], (1, 0)).astype(BF16)
    for g in range(n_out):
        cols = slice(g * channels, (g + 1) * channels)
        value = jnp.dot(lhs, weights[:, cols].astype(BF16), preferred_element_type=F32) + bias_ref[...]
        t0_ref[:, cols] = value
        mine = value[2 * width : (2 + own) * width]
        stats_ref[g : g + 1, :] = mine.sum(0, keepdims=True)
        stats_ref[n_out + g : n_out + g + 1, :] = (mine * mine).sum(0, keepdims=True)


def lift(meta, weight, bias, latents, own, half, n_frames, n_out):
    _, each, size = latents.shape
    channels = bias.shape[0]
    pixels = (own + 4) * 2 * half
    stat_rows = -(-2 * n_out // 8) * 8
    depth = -(-9 * n_frames * each // 256) * 256
    return pl.pallas_call(
        functools.partial(lift_kernel, own=own, half=half, n_frames=n_frames, n_out=n_out),
        out_shape=(
            pltpu.VMEM((pixels, n_out * channels), F32),
            jax.ShapeDtypeStruct((stat_rows, channels), F32),
        ),
        in_specs=[SMEM] + [VMEM] * 3,
        out_specs=(VMEM, VMEM),
        scratch_shapes=[
            pltpu.VMEM((n_frames * each, size), F32),
            pltpu.VMEM((depth, pixels), F32),
            pltpu.VMEM((depth, n_out * channels), F32),
        ],
        compiler_params=params(20),
        cost_estimate=cost(8e9),
        name="lift",
    )(meta, weight.reshape(27, each, channels), bias.reshape(1, channels), latents)


def pair_weight_copies(w_hbm, wv, sems, channels):
    copies = []
    for c in range(2):
        for j in range(3):
            target = wv.at[:, pl.ds((j + c) * channels, channels), pl.ds(c * channels, channels)]
            copies.append(pltpu.make_async_copy(w_hbm.at[:, j], target, sems.at[3 * c + j]))
    return copies


def clear_pair_weights(wv, channels):
    zero = jnp.zeros((wv.shape[0], channels, channels), BF16)
    wv[:, 3 * channels : 4 * channels, 0:channels] = zero
    wv[:, 0:channels, channels : 2 * channels] = zero


def time1_kernel(
    meta, s0, s1, s2, s3, gain, shift, ts, w_hbm, t1v, stats_ref, slots, wv, wsems,
    *, count, per_group, n_blocks, own, n_out,
):
    frames, lines, half, _ = slots.shape
    channels = gain.shape[1]
    width = 2 * half
    weight_loads = pair_weight_copies(w_hbm, wv, wsems, channels)
    for copy in weight_loads:
        copy.start()
    clear_pair_weights(wv, channels)
    scale, move = half_affine((s0, s1, s2, s3), frames, gain[...], shift[...], count, per_group)
    first_line = meta[0] * own - 2
    for k in range(frames):
        cols = slice(k * channels, (k + 1) * channels)

        def norm(r, _, k=k, cols=cols):
            line = first_line + r
            inside = (line >= 0) & (line < n_blocks * own) & (meta[1] >= k)
            at = pl.multiple_of(r * width, width)
            even = half_silu(ts[pl.ds(at, half), cols], scale[k : k + 1], move[k : k + 1])
            odd = half_silu(ts[pl.ds(at + half, half), cols], scale[k : k + 1], move[k : k + 1])
            even = jnp.where(inside, even, 0.0)
            odd = jnp.where(inside, odd, 0.0)
            spread_columns(slots.at[k], r, 0, even, odd, channels)
            return 0

        lax.fori_loop(0, lines, norm, 0)
    for copy in weight_loads:
        copy.wait()
    out_lines = lines - 2
    for k in range(n_out):
        acc = None
        for t in range(3):
            for i in range(3):
                lhs = slots[k + 2 - t, i : i + out_lines].reshape(out_lines * half, 4 * channels)
                part = jnp.dot(lhs, wv[3 * t + i], preferred_element_type=F32)
                acc = part if acc is None else acc + part
        t1v[k] = acc.reshape(out_lines, half, 2 * channels)
        mine = acc[half : (1 + own) * half]
        first = mine.sum(0, keepdims=True)
        second = (mine * mine).sum(0, keepdims=True)
        stats_ref[k : k + 1, :] = first[:, :channels] + first[:, channels:]
        stats_ref[n_out + k : n_out + k + 1, :] = second[:, :channels] + second[:, channels:]


def time1(meta, stats, gain, shift, t0, weight, n_blocks, own, half, n_frames, n_out):
    channels = gain.shape[0]
    count = float(n_blocks * own * 2 * half * (channels // GROUPS))
    lines = own + 4
    return pl.pallas_call(
        functools.partial(
            time1_kernel, count=count, per_group=channels // GROUPS, n_blocks=n_blocks, own=own, n_out=n_out
        ),
        out_shape=(
            pltpu.VMEM((n_out, lines - 2, half, 2 * channels), F32),
            jax.ShapeDtypeStruct((-(-2 * n_out // 8) * 8, channels), F32),
        ),
        in_specs=[SMEM] + [VMEM] * 7 + [HBM],
        out_specs=(VMEM, VMEM),
        scratch_shapes=[
            pltpu.VMEM((n_frames, lines, half, 4 * channels), BF16),
            pltpu.VMEM((9, 4 * channels, 2 * channels), BF16),
            pltpu.SemaphoreType.DMA((6,)),
        ],
        compiler_params=params(26),
        cost_estimate=cost(30e9),
        name="time1",
    )(meta, *stats, gain.reshape(1, channels), shift.reshape(1, channels), t0,
      in_hbm(weight.reshape(9, 3, channels, channels)))


def time2_kernel(
    meta, s0, s1, s2, s3, gain, shift, bias, ts, t0s, w_hbm, outv, slots, wv, rowf, wsems,
    *, count, per_group, n_blocks,
):
    frames, lines, half, _ = slots.shape
    own = lines - 2
    channels = gain.shape[1]
    width = 2 * half
    weight_loads = pair_weight_copies(w_hbm, wv, wsems, channels)
    for copy in weight_loads:
        copy.start()
    clear_pair_weights(wv, channels)
    scale, move = half_affine((s0, s1, s2, s3), frames, gain[...], shift[...], count, per_group)
    first_line = meta[0] * own - 1
    for k in range(frames):

        def norm(r, _, k=k):
            line = first_line + r
            inside = (line >= 0) & (line < n_blocks * own) & (meta[1] >= k)
            even = half_silu(ts[k, r, :, 0:channels], scale[k : k + 1], move[k : k + 1])
            odd = half_silu(ts[k, r, :, channels : 2 * channels], scale[k : k + 1], move[k : k + 1])
            even = jnp.where(inside, even, 0.0)
            odd = jnp.where(inside, odd, 0.0)
            spread_columns(slots.at[k], r, 0, even, odd, channels)
            return 0

        lax.fori_loop(0, lines, norm, 0)
    for copy in weight_loads:
        copy.wait()
    acc = None
    for t in range(3):
        for i in range(3):
            lhs = slots[2 - t, i : i + own].reshape(own * half, 4 * channels)
            part = jnp.dot(lhs, wv[3 * t + i], preferred_element_type=F32)
            acc = part if acc is None else acc + part
    acc = acc.reshape(own, half, 2 * channels)
    for r in range(own):
        for parity in range(2):
            at = (2 + r) * width + parity * half
            value = acc[r, :, parity * channels : (parity + 1) * channels] + bias[...]
            rowf[r, pl.ds(parity, half, stride=2), :] = value + t0s[at : at + half, 0:channels]
        outv[0, r] = rowf[r].astype(BF16)


def time2(meta, stats, gain, shift, bias, t1, t0, weight, n_blocks):
    frames, lines, half, _ = t1.shape
    own = lines - 2
    channels = gain.shape[0]
    count = float(n_blocks * own * 2 * half * (channels // GROUPS))
    return pl.pallas_call(
        functools.partial(time2_kernel, count=count, per_group=channels // GROUPS, n_blocks=n_blocks),
        out_shape=jax.ShapeDtypeStruct((1, own, 2 * half, channels), BF16),
        in_specs=[SMEM] + [VMEM] * 9 + [HBM],
        out_specs=VMEM,
        scratch_shapes=[
            pltpu.VMEM((frames, lines, half, 4 * channels), BF16),
            pltpu.VMEM((9, 4 * channels, 2 * channels), BF16),
            pltpu.VMEM((own, 2 * half, channels), F32),
            pltpu.SemaphoreType.DMA((6,)),
        ],
        compiler_params=params(24),
        cost_estimate=cost(12e9),
        name="time2",
    )(meta, *stats, gain.reshape(1, channels), shift.reshape(1, channels), bias.reshape(1, channels), t1, t0,
      in_hbm(weight.reshape(9, 3, channels, channels)))


def turned(block, axis, distance):
    count = lax.axis_size(axis)
    return lax.ppermute(block, axis, [(i, (i + distance) % count) for i in range(count)])


def from_all(block):
    return [block] + [turned(block, "rows", d) for d in range(1, lax.axis_size("rows"))]


def body(
    video, norm1_gain, norm1_shift, conv1_weight, conv1_bias, norm2_gain, norm2_shift, conv2_weight, conv2_bias,
    out_gain, out_shift, out_weight, out_bias, quant_weight, quant_bias, time_in_weight, time_in_bias,
    tnorm1_gain, tnorm1_shift, time1_weight, tnorm2_gain, tnorm2_shift, time2_weight, time2_bias,
):
    x = video[0]
    own, width, _ = x.shape
    half = width // 2
    n_blocks = lax.axis_size("rows")
    meta = jnp.stack([lax.axis_index("rows"), lax.axis_index("frames")]).astype(jnp.int32)
    up = turned(x[own - 2 :], "rows", 1)
    low = turned(x[:2], "rows", -1)
    stats = from_all(input_sums(x))
    h, xp, sums = conv1(meta, stats, norm1_gain, norm1_shift, conv1_bias, x, up, low, conv1_weight, n_blocks)
    y, sums = conv2(meta, from_all(sums), norm2_gain, norm2_shift, conv2_bias, h, xp, conv2_weight, n_blocks)
    part, to_up, to_low = head(
        meta, from_all(sums), out_gain, out_shift, y, out_weight, out_bias, quant_weight, quant_bias, n_blocks, 4
    )
    above = turned(to_low, "rows", 1)
    below = turned(to_up, "rows", -1)
    size = -(-((own + 6) * width) // LANES) * LANES
    row = lax.axis_index("rows")
    above = jnp.where(row > 0, above, 0.0)
    below = jnp.where(row < n_blocks - 1, below, 0.0)
    latent = (
        jnp.pad(part, ((0, 0), (2 * width, size))) [:, :size]
        + jnp.pad(above, ((0, 0), (0, size - 4 * width)))
        + jnp.pad(below, ((0, 0), ((own + 2) * width, size - (own + 6) * width)))
    ).astype(BF16)
    n_frames = lax.axis_size("frames")
    latents = lax.all_to_all(jnp.broadcast_to(latent[None], (n_frames,) + latent.shape), "frames", 0, 0)
    t0, sums = lift(meta, time_in_weight, time_in_bias, latents, own, half, 7, 5)
    t1, sums = time1(meta, from_all(sums), tnorm1_gain, tnorm1_shift, t0, time1_weight, n_blocks, own, half, 5, 3)
    return time2(meta, from_all(sums), tnorm2_gain, tnorm2_shift, time2_bias, t1, t0, time2_weight, n_blocks)


def solution(mesh):
    return jax.shard_map(
        body,
        mesh=mesh,
        in_specs=(P("frames", "rows", None, None),) + (P(),) * 23,
        out_specs=P("frames", "rows", None, None),
        check_vma=False,
    )
```

```python
import functools

import jax
import jax.numpy as jnp
from jax import lax
from jax.experimental import pallas as pl
from jax.experimental.pallas import tpu as pltpu
from jax.sharding import PartitionSpec as P

GROUPS = 32
EPS = 1e-06
LATENT_SCALE = 0.13025
LANES = 128
F32 = jnp.float32
BF16 = jnp.bfloat16

HBM = pl.BlockSpec(memory_space=pltpu.HBM)
VMEM = pl.BlockSpec(memory_space=pltpu.VMEM)
SMEM = pl.BlockSpec(memory_space=pltpu.SMEM)


def in_hbm(array):
    return pltpu.with_memory_space_constraint(array, pltpu.HBM)


def params(mib=48):
    return pltpu.CompilerParams(vmem_limit_bytes=mib * 1024 * 1024)


def cost(flops):
    return pl.CostEstimate(flops=int(flops), transcendentals=0, bytes_accessed=0)


def lane_groups(values, size):
    lane = lax.broadcasted_iota(jnp.int32, values.shape, 1)
    step = 1
    while step < size:
        up = pltpu.roll(values, step, 1)
        down = pltpu.roll(values, LANES - step, 1)
        values = values + jnp.where((lane & step) != 0, up, down)
        step *= 2
    return values


def half_affine(parts, rows, gain, shift, count, per_group):
    total = parts[0][...]
    for part in parts[1:]:
        total = total + part[...]
    total = lane_groups(total, per_group) / count
    mean = total[0:rows]
    variance = total[rows : 2 * rows] - mean * mean
    scale = lax.rsqrt(variance + EPS) * gain
    return 0.5 * scale, 0.5 * (shift - mean * scale)


def as_row(block):
    return jnp.concatenate([block[k : k + 1, :] for k in range(block.shape[0])], axis=1)


def half_silu(values, scale, shift):
    t = values * scale + shift
    return t * jnp.tanh(t) + t


def put_sums(out_ref, first, second, rows):
    for k in range(rows):
        lanes = slice(k * LANES, (k + 1) * LANES)
        out_ref[k : k + 1, :] = first[:, lanes]
        out_ref[rows + k : rows + k + 1, :] = second[:, lanes]


def spread_columns(slots, row, at, even, odd, channels):
    half, width = even.shape
    index = lax.broadcasted_iota(jnp.int32, (half, width), 0)
    before = jnp.where(index == 0, 0.0, pltpu.roll(odd, 1, 0))
    after = jnp.where(index == half - 1, 0.0, pltpu.roll(even, half - 1, 0))
    for slot, piece in enumerate((before, even, odd, after)):
        slots[row, :, slot * channels + at : slot * channels + at + width] = piece.astype(BF16)


def input_sums_kernel(x_hbm, x_ref, top_ref, bottom_ref, out_ref, sems):
    lines, width, channels = x_ref.shape
    halo = top_ref.shape[0]
    rows = channels // LANES
    copies = [pltpu.make_async_copy(x_hbm.at[r], x_ref.at[r], sems.at[r]) for r in range(lines)]
    for copy in copies:
        copy.start()
    first = [jnp.zeros((8, LANES), F32) for _ in range(rows)]
    second = list(first)
    for r in range(lines):
        copies[r].wait()
        for k in range(rows):
            v = x_ref[r, :, k * LANES : (k + 1) * LANES].astype(F32).reshape(width // 8, 8, LANES)
            first[k] = first[k] + v.sum(0)
            second[k] = second[k] + (v * v).sum(0)
        if r < halo:
            top_ref[r] = x_ref[r]
        if r >= lines - halo:
            bottom_ref[r - (lines - halo)] = x_ref[r]
    for k in range(rows):
        out_ref[k : k + 1, :] = first[k].sum(0, keepdims=True)
        out_ref[rows + k : rows + k + 1, :] = second[k].sum(0, keepdims=True)


def input_sums(x, halo):
    lines, width, channels = x.shape
    edge = pltpu.VMEM((halo, width, channels), BF16)
    return pl.pallas_call(
        input_sums_kernel,
        out_shape=(pltpu.VMEM(x.shape, BF16), edge, edge, jax.ShapeDtypeStruct((2 * channels // LANES, LANES), F32)),
        in_specs=[HBM],
        out_specs=(VMEM, VMEM, VMEM, VMEM),
        scratch_shapes=[pltpu.SemaphoreType.DMA((lines,))],
        compiler_params=params(8),
        cost_estimate=cost(6e9),
        name="input_sums",
    )(in_hbm(x))


def norm_line(slots, row, read, scale, move, inside, channels, keep=None):
    for at in range(0, channels, LANES):
        cols = slice(at, at + LANES)
        even, odd = read(at // LANES, cols)
        if keep is not None:
            keep[0, :, cols] = even.astype(BF16)
            keep[1, :, cols] = odd.astype(BF16)
        even = jnp.where(inside, half_silu(even, scale[:, cols], move[:, cols]), 0.0)
        odd = jnp.where(inside, half_silu(odd, scale[:, cols], move[:, cols]), 0.0)
        spread_columns(slots, row, at, even, odd, channels)


def block_conv(slots, weights, first, lines, channels, between=(), waits=None):
    half = slots.shape[1]
    acc = None
    for i in range(3):

        def dot(j, taps, i=i):
            parts = [
                slots[first + i : first + i + lines, :, (p + j) * channels : (p + j + taps) * channels].reshape(
                    lines * half, taps * channels
                )
                for p in range(2)
            ]
            tap_weights = weights[i, j * channels : (j + taps) * channels, :]
            return jnp.dot(jnp.concatenate(parts, axis=0), tap_weights, preferred_element_type=F32)

        if waits is None:
            part = dot(0, 3)
        else:
            part = None
            for j in range(3):
                waits[3 * i + j].wait()
                one = dot(j, 1)
                part = one if part is None else part + one
        acc = part if acc is None else acc + part
        if i < len(between):
            between[i]()
    return acc.reshape(2, lines, half, channels)


class Sums:
    def __init__(self, channels):
        self.channels = channels
        self.first = jnp.zeros((8, channels), F32)
        self.second = jnp.zeros((8, channels), F32)

    def add(self, line):
        line = line.reshape(-1, 8, self.channels)
        self.first = self.first + line.sum(0)
        self.second = self.second + (line * line).sum(0)

    def put(self, out_ref, base=None):
        rows = self.channels // LANES
        put_sums(out_ref, self.first.sum(0, keepdims=True), self.second.sum(0, keepdims=True), rows)
        if base is not None:
            out_ref[...] += base[...]


def conv1a_kernel(
    s0, s1, s2, s3, gain, shift, bias, x_ref, w_hbm, h_ref, xp_ref, slots, wv, stats_ref, rowf, wsems,
    *, halo, count, per_group,
):
    own, width, channels = x_ref.shape
    half = width // 2
    loads = []
    for i in range(3):
        for j in range(3):
            rows = pl.ds(j * channels, channels)
            loads.append(pltpu.make_async_copy(w_hbm.at[i, rows], wv.at[i, rows], wsems.at[3 * i + j]))
            loads[-1].start()
    scale, move = half_affine((s0, s1, s2, s3), channels // LANES, gain[...], shift[...], count, per_group)
    scale, move = as_row(scale), as_row(move)
    offset = bias[...].reshape(1, 1, 1, channels)

    def norm(r):
        def read(chunk, cols):
            rowf[r, chunk] = x_ref[r, :, cols].astype(F32)
            return rowf[r, chunk, pl.ds(0, half, stride=2), :], rowf[r, chunk, pl.ds(1, half, stride=2), :]

        norm_line(slots, halo + r, read, scale, move, True, channels, xp_ref.at[r])

    sums = Sums(channels)
    norm(0)
    norm(1)
    for b in range(0, own - 2, 2):
        lines = [functools.partial(norm, r) for r in (range(2, 6) if b == 0 else range(b + 4, b + 6)) if r < own]
        acc = block_conv(slots, wv, halo + b, 2, channels, lines[:2], loads if b == 0 else None) + offset
        for line in lines[2:]:
            line()
        for r in range(2):
            for p in range(2):
                h_ref[halo + b + r, p] = acc[p, r]
                sums.add(acc[p, r])
    sums.put(stats_ref)


def conv1b_kernel(
    meta, s0, s1, s2, s3, gain, shift, bias, up_ref, low_ref, base, wv, h_in, slots_in,
    h_ref, slots, stats_ref, rowf, *, count, per_group, n_blocks,
):
    halo, width, channels = up_ref.shape
    half = width // 2
    lines = slots.shape[0]
    scale, move = half_affine((s0, s1, s2, s3), channels // LANES, gain[...], shift[...], count, per_group)
    scale, move = as_row(scale), as_row(move)
    offset = bias[...].reshape(1, 1, 1, channels)
    sums = Sums(channels)

    def norm(source, r, inside, at):
        def read(chunk, cols):
            rowf[at, chunk] = source[r, :, cols].astype(F32)
            return rowf[at, chunk, pl.ds(0, half, stride=2), :], rowf[at, chunk, pl.ds(1, half, stride=2), :]

        norm_line(slots, at, read, scale, move, inside, channels)

    for r in range(halo):
        norm(up_ref, r, meta[0] > 0, r)
    later = [functools.partial(norm, low_ref, r, meta[0] < n_blocks - 1, lines - halo + r) for r in range(halo)]
    for first, mine in ((0, 1), (lines - 4, 0)):
        acc = block_conv(slots, wv, first, 2, channels, later if first == 0 else ()) + offset
        for r in range(2):
            for p in range(2):
                h_ref[first + r, p] = acc[p, r]
                if r == mine:
                    sums.add(acc[p, r])
    sums.put(stats_ref, base)


def conv1(meta, stats, gain, shift, bias, x, up, low, weight, n_blocks):
    own, width, channels = x.shape
    halo = up.shape[0]
    lines = own + 2 * halo
    half = width // 2
    rows = channels // LANES
    settings = dict(count=float(n_blocks * own * width * (channels // GROUPS)), per_group=channels // GROUPS)
    gain, shift, bias = gain.reshape(rows, LANES), shift.reshape(rows, LANES), bias.reshape(1, channels)
    h_type = pltpu.VMEM((lines - 2, 2, half, channels), F32)
    slots_type = pltpu.VMEM((lines, half, 4 * channels), BF16)
    stats_type = jax.ShapeDtypeStruct((2 * rows, LANES), F32)
    h, xp, slots, wv, base = pl.pallas_call(
        functools.partial(conv1a_kernel, halo=halo, **settings),
        out_shape=(
            h_type,
            pltpu.VMEM((own, 2, half, channels), BF16),
            slots_type,
            pltpu.VMEM((3, 3 * channels, channels), BF16),
            stats_type,
        ),
        in_specs=[VMEM] * 8 + [HBM],
        out_specs=(VMEM,) * 5,
        scratch_shapes=[
            pltpu.VMEM((own, channels // LANES, width, LANES), F32),
            pltpu.SemaphoreType.DMA((9,)),
        ],
        compiler_params=params(26),
        cost_estimate=cost(25e9),
        name="conv1a",
    )(*stats, gain, shift, bias, x, in_hbm(weight.reshape(3, 3 * channels, channels)))
    h, _, sums = pl.pallas_call(
        functools.partial(conv1b_kernel, n_blocks=n_blocks, **settings),
        out_shape=(h_type, slots_type, stats_type),
        in_specs=[SMEM] + [VMEM] * 13,
        out_specs=(VMEM,) * 3,
        scratch_shapes=[pltpu.VMEM((lines, channels // LANES, width, LANES), F32)],
        input_output_aliases={12: 0, 13: 1},
        compiler_params=params(26),
        cost_estimate=cost(20e9),
        name="conv1b",
    )(meta, *stats, gain, shift, bias, up, low, base, wv, h, slots)
    return h, xp, sums


def conv2_kernel(
    meta, s0, s1, s2, s3, gain, shift, bias, hs, xs, wv, y_ref, stats_ref, slots,
    *, count, per_group, n_blocks,
):
    lines, _, half, channels = hs.shape
    own = lines - 2
    scale, move = half_affine((s0, s1, s2, s3), channels // LANES, gain[...], shift[...], count, per_group)
    scale, move = as_row(scale), as_row(move)
    offset = bias[...].reshape(1, 1, 1, channels)

    def norm(r):
        inside = True
        if r == 0:
            inside = meta[0] > 0
        if r == lines - 1:
            inside = meta[0] < n_blocks - 1
        norm_line(slots, r, lambda chunk, cols: (hs[r, 0, :, cols], hs[r, 1, :, cols]), scale, move, inside, channels)

    sums = Sums(channels)
    norm(0)
    norm(1)
    for b in range(0, own, 2):
        ahead = [functools.partial(norm, r) for r in (range(2, 6) if b == 0 else range(b + 4, b + 6)) if r < lines]
        acc = block_conv(slots, wv, b, 2, channels, ahead[:2]) + offset
        for line in ahead[2:]:
            line()
        for r in range(2):
            for p in range(2):
                value = acc[p, r] + xs[b + r, p].astype(F32)
                y_ref[b + r, p] = value
                sums.add(value)
    sums.put(stats_ref)


def conv2(meta, stats, gain, shift, bias, h, xp, weight, n_blocks):
    lines, _, half, channels = h.shape
    own = lines - 2
    rows = channels // LANES
    count = float(n_blocks * own * 2 * half * (channels // GROUPS))
    return pl.pallas_call(
        functools.partial(conv2_kernel, count=count, per_group=channels // GROUPS, n_blocks=n_blocks),
        out_shape=(
            pltpu.VMEM((own, 2, half, channels), F32),
            jax.ShapeDtypeStruct((2 * rows, LANES), F32),
        ),
        in_specs=[SMEM] + [VMEM] * 10,
        out_specs=(VMEM, VMEM),
        scratch_shapes=[pltpu.VMEM((lines, half, 4 * channels), BF16)],
        compiler_params=params(26),
        cost_estimate=cost(30e9),
        name="conv2",
    )(meta, *stats, gain.reshape(rows, LANES), shift.reshape(rows, LANES), bias.reshape(1, channels), h, xp,
      weight.reshape(3, 3 * channels, channels))


def column_shift(values, tap, half):
    size = values.shape[1]
    lane = lax.broadcasted_iota(jnp.int32, values.shape, 1) % (2 * half)
    even = lane < half
    if tap == 0:
        moved = jnp.where(even, pltpu.roll(values, size - (half - 1), 1), pltpu.roll(values, half, 1))
        return jnp.where(lane == 0, 0.0, moved)
    moved = jnp.where(even, pltpu.roll(values, size - half, 1), pltpu.roll(values, half - 1, 1))
    return jnp.where(lane == 2 * half - 1, 0.0, moved)


def head_kernel(
    meta, s0, s1, s2, s3, gain, shift, w_ref, b_ref, q_ref, qb_ref, ys, part_ref, up_ref, low_ref, act,
    *, count, per_group, n_blocks, n_send,
):
    own, _, half, channels = ys.shape
    width = 2 * half
    scale, move = half_affine((s0, s1, s2, s3), channels // LANES, gain[...], shift[...], count, per_group)
    scale, move = as_row(scale), as_row(move)

    def norm(r, _):
        for parity in range(2):
            for at in range(0, channels, LANES):
                cols = slice(at, at + LANES)
                act[r, parity, :, cols] = half_silu(ys[r, parity, :, cols], scale[:, cols], move[:, cols]).astype(BF16)
        return 0

    lax.fori_loop(0, own, norm, 0)
    flat = act[...].reshape(own * width, channels)
    taps = lax.dot_general(w_ref[...], flat, (((1,), (1,)), ((), ())), preferred_element_type=F32)
    size = part_ref.shape[1]
    moments_n = taps.shape[0] // 9
    spare = jnp.zeros((moments_n, size - own * width), F32)
    total = None
    for i in range(3):
        piece = None
        for j in range(3):
            at = (3 * i + j) * moments_n
            one = taps[at : at + moments_n]
            one = one if j == 1 else column_shift(one, j, half)
            piece = one if piece is None else piece + one
        piece = jnp.concatenate([piece, spare], axis=1)
        if i < 2:
            piece = pltpu.roll(piece, (2 - i) * width, 1)
        total = piece if total is None else total + piece
    lane = lax.broadcasted_iota(jnp.int32, (1, size), 1)
    own_lane = (lane >= width) & (lane < (own + 1) * width)
    latents = []
    for c in range(q_ref.shape[0]):
        value, offset = None, qb_ref[c]
        for o in range(moments_n):
            term = total[o : o + 1, :] * q_ref[c, o]
            value = term if value is None else value + term
            offset = offset + b_ref[o] * q_ref[c, o]
        latents.append(LATENT_SCALE * (value + jnp.where(own_lane, offset, 0.0)))
    latent = jnp.concatenate(latents, axis=0)
    keep = ((lane >= width) | (meta[0] > 0)) & ((lane < (own + 1) * width) | (meta[0] < n_blocks - 1))
    part_ref[...] = jnp.where(keep, latent, 0.0)
    up_ref[...] = latent[:, : n_send * width]
    low_ref[...] = pltpu.roll(latent, size - (own + 2 - n_send) * width, 1)[:, : n_send * width]


def head(meta, stats, gain, shift, y, weight, bias, quant_weight, quant_bias, n_blocks, n_send):
    own, _, half, channels = y.shape
    width = 2 * half
    rows = channels // LANES
    moments, latents = quant_weight.shape
    count = float(n_blocks * own * width * (channels // GROUPS))
    size = -(-((own + 2) * width) // LANES) * LANES
    taps = weight.transpose(0, 1, 3, 2).reshape(9 * moments, channels)
    return pl.pallas_call(
        functools.partial(head_kernel, count=count, per_group=channels // GROUPS, n_blocks=n_blocks, n_send=n_send),
        out_shape=(
            jax.ShapeDtypeStruct((latents, size), F32),
            jax.ShapeDtypeStruct((latents, n_send * width), F32),
            jax.ShapeDtypeStruct((latents, n_send * width), F32),
        ),
        in_specs=[SMEM] + [VMEM] * 7 + [SMEM] * 3 + [VMEM],
        out_specs=(VMEM, VMEM, VMEM),
        scratch_shapes=[pltpu.VMEM((own, 2, half, channels), BF16)],
        compiler_params=params(12),
        cost_estimate=cost(10e9),
        name="head",
    )(meta, *stats, gain.reshape(rows, LANES), shift.reshape(rows, LANES), taps, bias, quant_weight.T, quant_bias, y)


def lift_kernel(meta, w_ref, bias_ref, latents, t0_ref, stats_ref, stack, patches, weights, *, own, half, n_frames, n_out):
    width = 2 * half
    out_lines = own + 4
    pixels = out_lines * width
    depth, size = stack.shape
    each = latents.shape[1]
    channels = bias_ref.shape[1]
    for s in range(n_frames):
        frame = meta[1] - (n_frames - 1 - s)
        value = latents[jnp.maximum(frame, 0)].astype(F32)
        stack[s * each : (s + 1) * each, :] = jnp.where(frame >= 0, value, 0.0)
    frames = stack[...]
    patches[9 * depth :, :] = jnp.zeros_like(patches[9 * depth :, :])
    weights[...] = jnp.zeros_like(weights)
    for j in range(3):
        moved = frames if j == 1 else column_shift(frames, j, half)
        for i in range(3):
            piece = moved if i == 0 else pltpu.roll(moved, size - i * width, 1)
            at = (3 * i + j) * depth
            patches[at : at + depth, :] = piece[:, :pixels]
            for t in range(3):
                tap = w_ref[9 * t + 3 * i + j].astype(F32)
                for g in range(n_out):
                    row = at + (n_frames - 3 - g + t) * each
                    weights[row : row + each, g * channels : (g + 1) * channels] = tap
    lhs = jnp.transpose(patches[...], (1, 0)).astype(BF16)
    for g in range(n_out):
        cols = slice(g * channels, (g + 1) * channels)
        value = jnp.dot(lhs, weights[:, cols].astype(BF16), preferred_element_type=F32) + bias_ref[...]
        t0_ref[:, cols] = value
        mine = value[2 * width : (2 + own) * width]
        stats_ref[g : g + 1, :] = mine.sum(0, keepdims=True)
        stats_ref[n_out + g : n_out + g + 1, :] = (mine * mine).sum(0, keepdims=True)


def lift(meta, weight, bias, latents, own, half, n_frames, n_out):
    _, each, size = latents.shape
    channels = bias.shape[0]
    pixels = (own + 4) * 2 * half
    stat_rows = -(-2 * n_out // 8) * 8
    depth = -(-9 * n_frames * each // 256) * 256
    return pl.pallas_call(
        functools.partial(lift_kernel, own=own, half=half, n_frames=n_frames, n_out=n_out),
        out_shape=(
            pltpu.VMEM((pixels, n_out * channels), F32),
            jax.ShapeDtypeStruct((stat_rows, channels), F32),
        ),
        in_specs=[SMEM] + [VMEM] * 3,
        out_specs=(VMEM, VMEM),
        scratch_shapes=[
            pltpu.VMEM((n_frames * each, size), F32),
            pltpu.VMEM((depth, pixels), F32),
            pltpu.VMEM((depth, n_out * channels), F32),
        ],
        compiler_params=params(20),
        cost_estimate=cost(8e9),
        name="lift",
    )(meta, weight.reshape(27, each, channels), bias.reshape(1, channels), latents)


def pair_weights(w_ref, tap):
    first, second, third = (w_ref[tap, j] for j in range(3))
    none = jnp.zeros_like(first)
    rows = ((first, none), (second, first), (third, second), (none, third))
    return jnp.concatenate([jnp.concatenate(row, axis=1) for row in rows], axis=0)


class Ahead:
    def __init__(self, order, emit):
        self.order, self.emit, self.done = list(dict.fromkeys(order)), emit, set()

    def need(self, items):
        while not self.done.issuperset(items):
            self.more(1)

    def more(self, count):
        for _ in range(min(count, len(self.order))):
            item = self.order.pop(0)
            self.emit(*item)
            self.done.add(item)


def clip_blocks(slots, w_ref, blocks, lines, ahead, finish, pace):
    half, depth = slots.shape[2], slots.shape[3]
    for k, first in blocks:
        acc = None
        for t in range(3):
            frame = k + 2 - t
            ahead.need([(frame, r) for r in range(first, first + lines + 2)])
            for i in range(3):
                lhs = slots[frame, first + i : first + i + lines].reshape(lines * half, depth)
                part = jnp.dot(lhs, pair_weights(w_ref, 3 * t + i), preferred_element_type=F32)
                acc = part if acc is None else acc + part
            ahead.more(pace)
        finish(k, first, acc)


def block_order(blocks, lines):
    return [(k + 2 - t, r) for k, first in blocks for t in range(3) for r in range(first, first + lines + 2)]


def time1_kernel(
    meta, s0, s1, s2, s3, gain, shift, ts, w_ref, t1v, stats_ref, slots,
    *, count, per_group, n_blocks, own, n_out,
):
    frames, lines, half, _ = slots.shape
    channels = gain.shape[1]
    width = 2 * half
    scale, move = half_affine((s0, s1, s2, s3), frames, gain[...], shift[...], count, per_group)
    first_line = meta[0] * own - 2

    def norm(k, r):
        line = first_line + r
        inside = (line >= 0) & (line < n_blocks * own) & (meta[1] >= k)
        at = r * width
        cols = slice(k * channels, (k + 1) * channels)
        even = half_silu(ts[at : at + half, cols], scale[k : k + 1], move[k : k + 1])
        odd = half_silu(ts[at + half : at + width, cols], scale[k : k + 1], move[k : k + 1])
        spread_columns(slots.at[k], r, 0, jnp.where(inside, even, 0.0), jnp.where(inside, odd, 0.0), channels)

    part_lines = (lines - 2) // 2
    blocks = [(k, first) for first in (0, part_lines) for k in reversed(range(n_out))]
    sums = [[jnp.zeros((8, 2 * channels), F32)] * 2 for _ in range(n_out)]

    def finish(k, first, acc):
        t1v[k, first : first + part_lines] = acc.reshape(part_lines, half, 2 * channels)
        skip = 1 if first == 0 else 0
        mine = acc[skip * half : (skip + part_lines - 1) * half].reshape(-1, 8, 2 * channels)
        sums[k] = [sums[k][0] + mine.sum(0), sums[k][1] + (mine * mine).sum(0)]

    ahead = Ahead(block_order(blocks, part_lines), norm)
    clip_blocks(slots, w_ref, blocks, part_lines, ahead, finish, 4)
    for k in range(n_out):
        for at, value in enumerate(sums[k]):
            value = value.sum(0, keepdims=True)
            row = at * n_out + k
            stats_ref[row : row + 1, :] = value[:, :channels] + value[:, channels:]


def time1(meta, stats, gain, shift, t0, weight, n_blocks, own, half, n_frames, n_out):
    channels = gain.shape[0]
    count = float(n_blocks * own * 2 * half * (channels // GROUPS))
    lines = own + 4
    return pl.pallas_call(
        functools.partial(
            time1_kernel, count=count, per_group=channels // GROUPS, n_blocks=n_blocks, own=own, n_out=n_out
        ),
        out_shape=(
            pltpu.VMEM((n_out, lines - 2, half, 2 * channels), F32),
            jax.ShapeDtypeStruct((-(-2 * n_out // 8) * 8, channels), F32),
        ),
        in_specs=[SMEM] + [VMEM] * 8,
        out_specs=(VMEM, VMEM),
        scratch_shapes=[
            pltpu.VMEM((n_frames, lines, half, 4 * channels), BF16),
        ],
        compiler_params=params(26),
        cost_estimate=cost(30e9),
        name="time1",
    )(meta, *stats, gain.reshape(1, channels), shift.reshape(1, channels), t0,
      weight.reshape(9, 3, channels, channels))


def time2_kernel(
    meta, s0, s1, s2, s3, gain, shift, bias, ts, t0s, w_ref, outv, slots, rowf,
    *, count, per_group, n_blocks,
):
    frames, lines, half, _ = slots.shape
    own = lines - 2
    channels = gain.shape[1]
    width = 2 * half
    scale, move = half_affine((s0, s1, s2, s3), frames, gain[...], shift[...], count, per_group)
    first_line = meta[0] * own - 1

    def norm(k, r):
        line = first_line + r
        inside = (line >= 0) & (line < n_blocks * own) & (meta[1] >= k)
        even = half_silu(ts[k, r, :, 0:channels], scale[k : k + 1], move[k : k + 1])
        odd = half_silu(ts[k, r, :, channels : 2 * channels], scale[k : k + 1], move[k : k + 1])
        spread_columns(slots.at[k], r, 0, jnp.where(inside, even, 0.0), jnp.where(inside, odd, 0.0), channels)

    part_lines = own // 2
    blocks = [(0, 0), (0, part_lines)]

    def finish(k, first, acc):
        acc = acc.reshape(part_lines, half, 2 * channels)
        for r in range(part_lines):
            for parity in range(2):
                at = (2 + first + r) * width + parity * half
                value = acc[r, :, parity * channels : (parity + 1) * channels] + bias[...]
                rowf[first + r, pl.ds(parity, half, stride=2), :] = value + t0s[at : at + half, 0:channels]
            outv[0, first + r] = rowf[first + r].astype(BF16)

    ahead = Ahead(block_order(blocks, part_lines), norm)
    clip_blocks(slots, w_ref, blocks, part_lines, ahead, finish, 4)


def time2(meta, stats, gain, shift, bias, t1, t0, weight, n_blocks):
    frames, lines, half, _ = t1.shape
    own = lines - 2
    channels = gain.shape[0]
    count = float(n_blocks * own * 2 * half * (channels // GROUPS))
    return pl.pallas_call(
        functools.partial(time2_kernel, count=count, per_group=channels // GROUPS, n_blocks=n_blocks),
        out_shape=jax.ShapeDtypeStruct((1, own, 2 * half, channels), BF16),
        in_specs=[SMEM] + [VMEM] * 10,
        out_specs=VMEM,
        scratch_shapes=[
            pltpu.VMEM((frames, lines, half, 4 * channels), BF16),
            pltpu.VMEM((own, 2 * half, channels), F32),
        ],
        compiler_params=params(24),
        cost_estimate=cost(12e9),
        name="time2",
    )(meta, *stats, gain.reshape(1, channels), shift.reshape(1, channels), bias.reshape(1, channels), t1, t0,
      weight.reshape(9, 3, channels, channels))


def turned(block, axis, distance):
    count = lax.axis_size(axis)
    return lax.ppermute(block, axis, [(i, (i + distance) % count) for i in range(count)])


def from_all(block):
    return [block] + [turned(block, "rows", d) for d in range(1, lax.axis_size("rows"))]


def body(
    video, norm1_gain, norm1_shift, conv1_weight, conv1_bias, norm2_gain, norm2_shift, conv2_weight, conv2_bias,
    out_gain, out_shift, out_weight, out_bias, quant_weight, quant_bias, time_in_weight, time_in_bias,
    tnorm1_gain, tnorm1_shift, time1_weight, tnorm2_gain, tnorm2_shift, time2_weight, time2_bias,
):
    x = video[0]
    own, width, _ = x.shape
    half = width // 2
    n_blocks = lax.axis_size("rows")
    meta = jnp.stack([lax.axis_index("rows"), lax.axis_index("frames")]).astype(jnp.int32)
    x, top, bottom, sums = input_sums(x, 2)
    stats = from_all(sums)
    up = turned(bottom, "rows", 1)
    low = turned(top, "rows", -1)
    h, xp, sums = conv1(meta, stats, norm1_gain, norm1_shift, conv1_bias, x, up, low, conv1_weight, n_blocks)
    y, sums = conv2(meta, from_all(sums), norm2_gain, norm2_shift, conv2_bias, h, xp, conv2_weight, n_blocks)
    part, to_up, to_low = head(
        meta, from_all(sums), out_gain, out_shift, y, out_weight, out_bias, quant_weight, quant_bias, n_blocks, 4
    )
    above = turned(to_low, "rows", 1)
    below = turned(to_up, "rows", -1)
    size = -(-((own + 6) * width) // LANES) * LANES
    row = lax.axis_index("rows")
    above = jnp.where(row > 0, above, 0.0)
    below = jnp.where(row < n_blocks - 1, below, 0.0)
    latent = (
        jnp.pad(part, ((0, 0), (2 * width, size))) [:, :size]
        + jnp.pad(above, ((0, 0), (0, size - 4 * width)))
        + jnp.pad(below, ((0, 0), ((own + 2) * width, size - (own + 6) * width)))
    ).astype(BF16)
    n_frames = lax.axis_size("frames")
    latents = lax.all_to_all(jnp.broadcast_to(latent[None], (n_frames,) + latent.shape), "frames", 0, 0)
    t0, sums = lift(meta, time_in_weight, time_in_bias, latents, own, half, 7, 5)
    t1, sums = time1(meta, from_all(sums), tnorm1_gain, tnorm1_shift, t0, time1_weight, n_blocks, own, half, 5, 3)
    return time2(meta, from_all(sums), tnorm2_gain, tnorm2_shift, time2_bias, t1, t0, time2_weight, n_blocks)


def solution(mesh):
    return jax.shard_map(
        body,
        mesh=mesh,
        in_specs=(P("frames", "rows", None, None),) + (P(),) * 23,
        out_specs=P("frames", "rows", None, None),
        check_vma=False,
    )
```

```python
import functools

import jax
import jax.numpy as jnp
from jax import lax
from jax.experimental import pallas as pl
from jax.experimental.pallas import tpu as pltpu
from jax.sharding import PartitionSpec as P


GROUPS = 32
EPS = 1e-06
LATENT_SCALE = 0.13025
LANES = 128
F32 = jnp.float32
BF16 = jnp.bfloat16

HBM = pl.BlockSpec(memory_space=pltpu.HBM)
VMEM = pl.BlockSpec(memory_space=pltpu.VMEM)
SMEM = pl.BlockSpec(memory_space=pltpu.SMEM)


def in_hbm(array):
    return pltpu.with_memory_space_constraint(array, pltpu.HBM)


def params(mib=48):
    return pltpu.CompilerParams(vmem_limit_bytes=mib * 1024 * 1024)


def cost(flops):
    return pl.CostEstimate(flops=int(flops), transcendentals=0, bytes_accessed=0)


def lane_groups(values, size):
    lane = lax.broadcasted_iota(jnp.int32, values.shape, 1)
    step = 1
    while step < size:
        up = pltpu.roll(values, step, 1)
        down = pltpu.roll(values, LANES - step, 1)
        values = values + jnp.where((lane & step) != 0, up, down)
        step *= 2
    return values


def half_affine(parts, rows, gain, shift, count, per_group):
    total = parts[0][...]
    for part in parts[1:]:
        total = total + part[...]
    total = lane_groups(total, per_group) / count
    mean = total[0:rows]
    variance = total[rows : 2 * rows] - mean * mean
    scale = lax.rsqrt(variance + EPS) * gain
    return 0.5 * scale, 0.5 * (shift - mean * scale)


def as_row(block):
    return jnp.concatenate([block[k : k + 1, :] for k in range(block.shape[0])], axis=1)


def half_silu(values, scale, shift):
    t = values * scale + shift
    return t * jnp.tanh(t) + t


def put_sums(out_ref, first, second, rows):
    for k in range(rows):
        lanes = slice(k * LANES, (k + 1) * LANES)
        out_ref[k : k + 1, :] = first[:, lanes]
        out_ref[rows + k : rows + k + 1, :] = second[:, lanes]


def spread_columns(slots, row, at, even, odd, channels):
    half, width = even.shape
    index = lax.broadcasted_iota(jnp.int32, (half, width), 0)
    before = jnp.where(index == 0, 0.0, pltpu.roll(odd, 1, 0))
    after = jnp.where(index == half - 1, 0.0, pltpu.roll(even, half - 1, 0))
    for slot, piece in enumerate((before, even, odd, after)):
        slots[row, :, slot * channels + at : slot * channels + at + width] = piece.astype(BF16)


def input_sums_kernel(meta, x_hbm, x_ref, near_ref, far_ref, out_ref, sems):
    lines, width, channels = x_ref.shape
    halo = near_ref.shape[0]
    rows = channels // LANES
    even = (meta[0] & 1) == 0
    copies = [pltpu.make_async_copy(x_hbm.at[r], x_ref.at[r], sems.at[r]) for r in range(lines)]
    for copy in copies:
        copy.start()
    first = [jnp.zeros((8, LANES), F32) for _ in range(rows)]
    second = list(first)
    for r in range(lines):
        copies[r].wait()
        for k in range(rows):
            v = x_ref[r, :, k * LANES : (k + 1) * LANES].astype(F32).reshape(width // 8, 8, LANES)
            first[k] = first[k] + v.sum(0)
            second[k] = second[k] + (v * v).sum(0)
    for r in range(halo):
        top, bottom = x_ref[r], x_ref[lines - halo + r]
        near_ref[r] = jnp.where(even, bottom, top)
        far_ref[r] = jnp.where(even, top, bottom)
    for k in range(rows):
        out_ref[k : k + 1, :] = first[k].sum(0, keepdims=True)
        out_ref[rows + k : rows + k + 1, :] = second[k].sum(0, keepdims=True)


def input_sums(meta, x, halo):
    lines, width, channels = x.shape
    edge = pltpu.VMEM((halo, width, channels), BF16)
    return pl.pallas_call(
        input_sums_kernel,
        out_shape=(
            pltpu.VMEM(x.shape, BF16),
            edge,
            edge,
            jax.ShapeDtypeStruct((2 * channels // LANES, LANES), F32),
        ),
        in_specs=[SMEM, HBM],
        out_specs=(VMEM,) * 4,
        scratch_shapes=[pltpu.SemaphoreType.DMA((lines,))],
        compiler_params=params(8),
        cost_estimate=cost(6e9),
        name="input_sums",
    )(meta, in_hbm(x))


def norm_line(slots, row, read, scale, move, inside, channels, keep=None):
    for at in range(0, channels, LANES):
        cols = slice(at, at + LANES)
        even, odd = read(at // LANES, cols)
        if keep is not None:
            keep[0, :, cols] = even.astype(BF16)
            keep[1, :, cols] = odd.astype(BF16)
        even = jnp.where(inside, half_silu(even, scale[:, cols], move[:, cols]), 0.0)
        odd = jnp.where(inside, half_silu(odd, scale[:, cols], move[:, cols]), 0.0)
        spread_columns(slots, row, at, even, odd, channels)


def block_conv(slots, weights, firsts, lines, channels, between=()):
    half = slots.shape[1]
    acc = None
    for i in range(3):
        parts = [
            slots[f + i : f + i + lines, :, p * channels : (p + 3) * channels].reshape(lines * half, 3 * channels)
            for p in range(2)
            for f in firsts
        ]
        part = jnp.dot(jnp.concatenate(parts, axis=0), weights[i], preferred_element_type=F32)
        acc = part if acc is None else acc + part
        if i < len(between):
            between[i]()
    return acc.reshape(2, len(firsts) * lines, half, channels)


class Sums:
    def __init__(self, channels):
        self.channels = channels
        self.first = jnp.zeros((8, channels), F32)
        self.second = jnp.zeros((8, channels), F32)

    def add(self, line):
        line = line.reshape(-1, 8, self.channels)
        self.first = self.first + line.sum(0)
        self.second = self.second + (line * line).sum(0)

    def put(self, out_ref, base=None):
        rows = self.channels // LANES
        put_sums(out_ref, self.first.sum(0, keepdims=True), self.second.sum(0, keepdims=True), rows)
        if base is not None:
            out_ref[...] += base[...]


def conv1_kernel(
    s0, s1, s2, s3, gain, shift, bias, x_ref, w_ref, h_ref, xp_ref, slots, stats_ref, rowf,
    *, halo, count, per_group,
):
    own, width, channels = x_ref.shape
    half = width // 2
    scale, move = half_affine((s0, s1, s2, s3), channels // LANES, gain[...], shift[...], count, per_group)
    scale, move = as_row(scale), as_row(move)
    offset = bias[...].reshape(1, 1, 1, channels)

    def norm(r):
        def read(chunk, cols):
            rowf[r, chunk] = x_ref[r, :, cols].astype(F32)
            return rowf[r, chunk, pl.ds(0, half, stride=2), :], rowf[r, chunk, pl.ds(1, half, stride=2), :]

        norm_line(slots, halo + r, read, scale, move, True, channels, xp_ref.at[r])

    sums = Sums(channels)
    norm(0)
    norm(1)
    for b in range(0, own - 2, 2):
        lines = [functools.partial(norm, r) for r in (range(2, 6) if b == 0 else range(b + 4, b + 6)) if r < own]
        acc = block_conv(slots, w_ref, [halo + b], 2, channels, lines[:2]) + offset
        for line in lines[2:]:
            line()
        for r in range(2):
            for p in range(2):
                h_ref[halo + b + r, p] = acc[p, r]
                sums.add(acc[p, r])
    sums.put(stats_ref)


def conv1_edge_kernel(
    meta, s0, s1, s2, s3, gain, shift, bias, near_ref, far_ref, base, w_ref, h_in, slots_in, h_ref, slots, *rest,
    distance, count, per_group, n_blocks,
):
    rowf = rest[-1]
    halo, width, channels = near_ref.shape
    half = width // 2
    lines = slots.shape[0]
    even_block = (meta[0] & 1) == 0
    scale, move = half_affine((s0, s1, s2, s3), channels // LANES, gain[...], shift[...], count, per_group)
    scale, move = as_row(scale), as_row(move)
    offset = bias[...].reshape(1, 1, 1, channels)

    def norm(above, r, inside, at, spare):
        def read(chunk, cols):
            near, far = near_ref[r, :, cols].astype(F32), far_ref[r, :, cols].astype(F32)
            rowf[spare, chunk] = jnp.where(even_block == above, far, near)
            return rowf[spare, chunk, pl.ds(0, half, stride=2), :], rowf[spare, chunk, pl.ds(1, half, stride=2), :]

        norm_line(slots, at, read, scale, move, inside, channels)

    top, bottom = halo - 1 - distance, lines - halo + distance
    norm(True, top, meta[0] > 0, top, 0)
    norm(False, distance, meta[0] < n_blocks - 1, bottom, 1)
    places = (top, bottom - 2)
    acc = block_conv(slots, w_ref, places, 1, channels) + offset
    sums = Sums(channels)
    for k, place in enumerate(places):
        for p in range(2):
            h_ref[place, p] = acc[p, k]
            if distance == 0:
                sums.add(acc[p, k])
    if distance == 0:
        sums.put(rest[0], base)


def conv1(meta, stats, gain, shift, bias, x, halos, weight, n_blocks):
    near, far = halos
    own, width, channels = x.shape
    halo = near.shape[0]
    lines = own + 2 * halo
    half = width // 2
    rows = channels // LANES
    settings = dict(count=float(n_blocks * own * width * (channels // GROUPS)), per_group=channels // GROUPS)
    gain, shift, bias = gain.reshape(rows, LANES), shift.reshape(rows, LANES), bias.reshape(1, channels)
    h_type = pltpu.VMEM((lines - 2, 2, half, channels), F32)
    slots_type = pltpu.VMEM((lines, half, 4 * channels), BF16)
    stats_type = jax.ShapeDtypeStruct((2 * rows, LANES), F32)
    h, xp, slots, base = pl.pallas_call(
        functools.partial(conv1_kernel, halo=halo, **settings),
        out_shape=(
            h_type,
            pltpu.VMEM((own, 2, half, channels), BF16),
            slots_type,
            stats_type,
        ),
        in_specs=[VMEM] * 9,
        out_specs=(VMEM,) * 4,
        scratch_shapes=[pltpu.VMEM((own, channels // LANES, width, LANES), F32)],
        compiler_params=params(26),
        cost_estimate=cost(25e9),
        name="conv1",
    )(*stats, gain, shift, bias, x, weight)

    def edge(distance, h, slots):
        return pl.pallas_call(
            functools.partial(conv1_edge_kernel, distance=distance, n_blocks=n_blocks, **settings),
            out_shape=(h_type, slots_type) + ((stats_type,) if distance == 0 else ()),
            in_specs=[SMEM] + [VMEM] * 13,
            out_specs=(VMEM,) * (3 if distance == 0 else 2),
            scratch_shapes=[pltpu.VMEM((2, channels // LANES, width, LANES), F32)],
            input_output_aliases={12: 0, 13: 1},
            compiler_params=params(26),
            cost_estimate=cost(10e9),
        )(meta, *stats, gain, shift, bias, near, far, base, weight, h, slots)

    h, slots, sums = edge(0, h, slots)
    return xp, sums, lambda: edge(1, h, slots)[0]


def conv2_kernel(
    meta, s0, s1, s2, s3, gain, shift, bias, hs, xs, wv, y_ref, stats_ref, slots,
    *, count, per_group, n_blocks,
):
    lines, _, _, channels = hs.shape
    own = lines - 2
    scale, move = half_affine((s0, s1, s2, s3), channels // LANES, gain[...], shift[...], count, per_group)
    scale, move = as_row(scale), as_row(move)
    offset = bias[...].reshape(1, 1, 1, channels)

    def norm(r):
        inside = True
        if r == 0:
            inside = meta[0] > 0
        if r == lines - 1:
            inside = meta[0] < n_blocks - 1
        norm_line(slots, r, lambda chunk, cols: (hs[r, 0, :, cols], hs[r, 1, :, cols]), scale, move, inside, channels)

    sums = Sums(channels)
    norm(0)
    norm(1)
    for b in range(0, own, 2):
        ahead = [functools.partial(norm, r) for r in (range(2, 6) if b == 0 else range(b + 4, b + 6)) if r < lines]
        acc = block_conv(slots, wv, [b], 2, channels, ahead[:2]) + offset
        for line in ahead[2:]:
            line()
        for r in range(2):
            for p in range(2):
                value = acc[p, r] + xs[b + r, p].astype(F32)
                y_ref[b + r, p] = value
                sums.add(value)
    sums.put(stats_ref)


def conv2(meta, stats, gain, shift, bias, h, xp, weight, n_blocks):
    lines, _, half, channels = h.shape
    own = lines - 2
    rows = channels // LANES
    count = float(n_blocks * own * 2 * half * (channels // GROUPS))
    return pl.pallas_call(
        functools.partial(conv2_kernel, count=count, per_group=channels // GROUPS, n_blocks=n_blocks),
        out_shape=(
            pltpu.VMEM((own, 2, half, channels), F32),
            jax.ShapeDtypeStruct((2 * rows, LANES), F32),
        ),
        in_specs=[SMEM] + [VMEM] * 10,
        out_specs=(VMEM, VMEM),
        scratch_shapes=[pltpu.VMEM((lines, half, 4 * channels), BF16)],
        compiler_params=params(26),
        cost_estimate=cost(30e9),
        name="conv2",
    )(meta, *stats, gain.reshape(rows, LANES), shift.reshape(rows, LANES), bias.reshape(1, channels), h, xp,
      weight.reshape(3, 3 * channels, channels))


def column_shift(values, tap, half):
    size = values.shape[1]
    lane = lax.broadcasted_iota(jnp.int32, values.shape, 1) % (2 * half)
    even = lane < half
    if tap == 0:
        moved = jnp.where(even, pltpu.roll(values, size - (half - 1), 1), pltpu.roll(values, half, 1))
        return jnp.where(lane == 0, 0.0, moved)
    moved = jnp.where(even, pltpu.roll(values, size - half, 1), pltpu.roll(values, half - 1, 1))
    return jnp.where(lane == 2 * half - 1, 0.0, moved)


def head_kernel(
    meta, s0, s1, s2, s3, gain, shift, w_ref, b_ref, q_ref, qb_ref, ys, part_ref, up_ref, low_ref, act,
    *, count, per_group, n_blocks, n_send,
):
    own, _, half, channels = ys.shape
    width = 2 * half
    scale, move = half_affine((s0, s1, s2, s3), channels // LANES, gain[...], shift[...], count, per_group)
    scale, move = as_row(scale), as_row(move)

    def norm(r, _):
        for parity in range(2):
            for at in range(0, channels, LANES):
                cols = slice(at, at + LANES)
                act[r, parity, :, cols] = half_silu(ys[r, parity, :, cols], scale[:, cols], move[:, cols]).astype(BF16)
        return 0

    lax.fori_loop(0, own, norm, 0)
    flat = act[...].reshape(own * width, channels)
    taps = lax.dot_general(w_ref[...], flat, (((1,), (1,)), ((), ())), preferred_element_type=F32)
    size = part_ref.shape[1]
    moments_n = taps.shape[0] // 9
    spare = jnp.zeros((moments_n, size - own * width), F32)
    total = None
    for i in range(3):
        piece = None
        for j in range(3):
            at = (3 * i + j) * moments_n
            one = taps[at : at + moments_n]
            one = one if j == 1 else column_shift(one, j, half)
            piece = one if piece is None else piece + one
        piece = jnp.concatenate([piece, spare], axis=1)
        if i < 2:
            piece = pltpu.roll(piece, (2 - i) * width, 1)
        total = piece if total is None else total + piece
    lane = lax.broadcasted_iota(jnp.int32, (1, size), 1)
    own_lane = (lane >= width) & (lane < (own + 1) * width)
    latents = []
    for c in range(q_ref.shape[0]):
        value, offset = None, qb_ref[c]
        for o in range(moments_n):
            term = total[o : o + 1, :] * q_ref[c, o]
            value = term if value is None else value + term
            offset = offset + b_ref[o] * q_ref[c, o]
        latents.append(LATENT_SCALE * (value + jnp.where(own_lane, offset, 0.0)))
    latent = jnp.concatenate(latents, axis=0)
    keep = ((lane >= width) | (meta[0] > 0)) & ((lane < (own + 1) * width) | (meta[0] < n_blocks - 1))
    part_ref[...] = jnp.where(keep, latent, 0.0)
    up_ref[...] = latent[:, : n_send * width]
    low_ref[...] = pltpu.roll(latent, size - (own + 2 - n_send) * width, 1)[:, : n_send * width]


def head(meta, stats, gain, shift, y, weight, bias, quant_weight, quant_bias, n_blocks, n_send):
    own, _, half, channels = y.shape
    width = 2 * half
    rows = channels // LANES
    moments, latents = quant_weight.shape
    count = float(n_blocks * own * width * (channels // GROUPS))
    size = -(-((own + 2) * width) // LANES) * LANES
    taps = weight.transpose(0, 1, 3, 2).reshape(9 * moments, channels)
    return pl.pallas_call(
        functools.partial(head_kernel, count=count, per_group=channels // GROUPS, n_blocks=n_blocks, n_send=n_send),
        out_shape=(
            jax.ShapeDtypeStruct((latents, size), F32),
            jax.ShapeDtypeStruct((latents, n_send * width), F32),
            jax.ShapeDtypeStruct((latents, n_send * width), F32),
        ),
        in_specs=[SMEM] + [VMEM] * 7 + [SMEM] * 3 + [VMEM],
        out_specs=(VMEM, VMEM, VMEM),
        scratch_shapes=[pltpu.VMEM((own, 2, half, channels), BF16)],
        compiler_params=params(12),
        cost_estimate=cost(10e9),
        name="head",
    )(meta, *stats, gain.reshape(rows, LANES), shift.reshape(rows, LANES), taps, bias, quant_weight.T, quant_bias, y)


def lift_kernel(meta, w_ref, bias_ref, latents, t0_ref, stats_ref, stack, patches, weights, *, own, half, n_frames, n_out):
    width = 2 * half
    out_lines = own + 4
    pixels = out_lines * width
    depth, size = stack.shape
    each = latents.shape[1]
    channels = bias_ref.shape[1]
    for s in range(n_frames):
        frame = meta[1] - (n_frames - 1 - s)
        value = latents[jnp.maximum(frame, 0)].astype(F32)
        stack[s * each : (s + 1) * each, :] = jnp.where(frame >= 0, value, 0.0)
    frames = stack[...]
    patches[9 * depth :, :] = jnp.zeros_like(patches[9 * depth :, :])
    weights[...] = jnp.zeros_like(weights)
    for j in range(3):
        moved = frames if j == 1 else column_shift(frames, j, half)
        for i in range(3):
            piece = moved if i == 0 else pltpu.roll(moved, size - i * width, 1)
            at = (3 * i + j) * depth
            patches[at : at + depth, :] = piece[:, :pixels]
            for t in range(3):
                tap = w_ref[9 * t + 3 * i + j].astype(F32)
                for g in range(n_out):
                    row = at + (n_frames - 3 - g + t) * each
                    weights[row : row + each, g * channels : (g + 1) * channels] = tap
    lhs = jnp.transpose(patches[...], (1, 0)).astype(BF16)
    for start in range(0, n_out, 2):
        pair = slice(start * channels, min(start + 2, n_out) * channels)
        values = jnp.dot(lhs, weights[:, pair].astype(BF16), preferred_element_type=F32)
        for g in range(start, min(start + 2, n_out)):
            value = values[:, (g - start) * channels : (g - start + 1) * channels] + bias_ref[...]
            t0_ref[:, g * channels : (g + 1) * channels] = value
            mine = value[2 * width : (2 + own) * width].reshape(-1, 8, channels)
            stats_ref[g : g + 1, :] = mine.sum(0).sum(0, keepdims=True)
            stats_ref[n_out + g : n_out + g + 1, :] = (mine * mine).sum(0).sum(0, keepdims=True)


def lift(meta, weight, bias, latents, own, half, n_frames, n_out):
    _, each, size = latents.shape
    channels = bias.shape[0]
    pixels = (own + 4) * 2 * half
    stat_rows = -(-2 * n_out // 8) * 8
    depth = -(-9 * n_frames * each // 256) * 256
    return pl.pallas_call(
        functools.partial(lift_kernel, own=own, half=half, n_frames=n_frames, n_out=n_out),
        out_shape=(
            pltpu.VMEM((pixels, n_out * channels), F32),
            jax.ShapeDtypeStruct((stat_rows, channels), F32),
        ),
        in_specs=[SMEM] + [VMEM] * 3,
        out_specs=(VMEM, VMEM),
        scratch_shapes=[
            pltpu.VMEM((n_frames * each, size), F32),
            pltpu.VMEM((depth, pixels), F32),
            pltpu.VMEM((depth, n_out * channels), F32),
        ],
        compiler_params=params(20),
        cost_estimate=cost(8e9),
        name="lift",
    )(meta, weight.reshape(27, each, channels), bias.reshape(1, channels), latents)


def pair_weights(w_ref, tap):
    first, second, third = (w_ref[tap, j] for j in range(3))
    none = jnp.zeros_like(first)
    rows = ((first, none), (second, first), (third, second), (none, third))
    return jnp.concatenate([jnp.concatenate(row, axis=1) for row in rows], axis=0)


class Ahead:
    def __init__(self, order, emit):
        self.order, self.emit, self.done = list(dict.fromkeys(order)), emit, set()

    def need(self, items):
        while not self.done.issuperset(items):
            self.more(1)

    def more(self, count):
        for _ in range(min(count, len(self.order))):
            item = self.order.pop(0)
            self.emit(*item)
            self.done.add(item)


def clip_blocks(slots, w_ref, blocks, lines, ahead, finish, pace):
    half, depth = slots.shape[2], slots.shape[3]
    for k, first in blocks:
        acc = None
        for t in range(3):
            frame = k + 2 - t
            ahead.need([(frame, r) for r in range(first, first + lines + 2)])
            for i in range(3):
                lhs = slots[frame, first + i : first + i + lines].reshape(lines * half, depth)
                part = jnp.dot(lhs, pair_weights(w_ref, 3 * t + i), preferred_element_type=F32)
                acc = part if acc is None else acc + part
            ahead.more(pace)
        finish(k, first, acc)


def block_order(blocks, lines):
    return [(k + 2 - t, r) for k, first in blocks for t in range(3) for r in range(first, first + lines + 2)]


def time1_line(ts, slots, meta, scale, move, n_blocks, own):
    half, depth = slots.shape[2], slots.shape[3]
    channels = depth // 4
    width = 2 * half

    def norm(k, r):
        line = meta[0] * own - 2 + r
        inside = meta[1] >= k
        if r < 2 or r >= own + 2:
            inside = inside & (line >= 0) & (line < n_blocks * own)
        at = r * width
        cols = slice(k * channels, (k + 1) * channels)
        even = half_silu(ts[at : at + half, cols], scale[k : k + 1], move[k : k + 1])
        odd = half_silu(ts[at + half : at + width, cols], scale[k : k + 1], move[k : k + 1])
        spread_columns(slots.at[k], r, 0, jnp.where(inside, even, 0.0), jnp.where(inside, odd, 0.0), channels)

    return norm


def time1_kernel(
    meta, s0, s1, s2, s3, gain, shift, ts, w_ref, t1v, slots, stats_ref, *, count, per_group, n_blocks, own, n_out,
):
    frames, _, half, _ = slots.shape
    channels = gain.shape[1]
    scale, move = half_affine((s0, s1, s2, s3), frames, gain[...], shift[...], count, per_group)
    norm = time1_line(ts, slots, meta, scale, move, n_blocks, own)
    part_lines = own // 2
    blocks = [(k, first) for first in (1, 1 + part_lines) for k in reversed(range(n_out))]
    sums = [[jnp.zeros((8, 2 * channels), F32)] * 2 for _ in range(n_out)]

    def finish(k, first, acc):
        t1v[k, first : first + part_lines] = acc.reshape(part_lines, half, 2 * channels)
        mine = acc.reshape(-1, 8, 2 * channels)
        sums[k] = [sums[k][0] + mine.sum(0), sums[k][1] + (mine * mine).sum(0)]

    ahead = Ahead(block_order(blocks, part_lines), norm)
    clip_blocks(slots, w_ref, blocks, part_lines, ahead, finish, 4)
    for k in range(n_out):
        for at, value in enumerate(sums[k]):
            value = value.sum(0, keepdims=True)
            row = at * n_out + k
            stats_ref[row : row + 1, :] = value[:, :channels] + value[:, channels:]


def time1_edge_kernel(
    meta, s0, s1, s2, s3, gain, shift, ts, w_ref, t1_in, slots_in, t1v, slots, *, count, per_group, n_blocks, own,
):
    frames, lines, half, _ = slots.shape
    n_out = t1v.shape[0]
    scale, move = half_affine((s0, s1, s2, s3), frames, gain[...], shift[...], count, per_group)
    norm = time1_line(ts, slots, meta, scale, move, n_blocks, own)
    ends = (0, lines - 1)
    ahead = Ahead([(k + 2 - t, r) for t in range(3) for k in range(n_out) for r in ends], norm)
    places = [(k, first) for k in range(n_out) for first in (0, lines - 3)]
    acc = None
    for t in range(3):
        ahead.need([(k + 2 - t, r) for k in range(n_out) for r in ends])
        for i in range(3):
            lhs = jnp.concatenate([slots[k + 2 - t, first + i] for k, first in places], axis=0)
            part = jnp.dot(lhs, pair_weights(w_ref, 3 * t + i), preferred_element_type=F32)
            acc = part if acc is None else acc + part
        ahead.more(2)
    for at, (k, first) in enumerate(places):
        t1v[k, first] = acc[at * half : (at + 1) * half]


def time1(meta, stats, gain, shift, t0, weight, n_blocks, own, half, n_frames, n_out):
    channels = gain.shape[0]
    lines = own + 4
    settings = dict(
        count=float(n_blocks * own * 2 * half * (channels // GROUPS)),
        per_group=channels // GROUPS,
        n_blocks=n_blocks,
        own=own,
    )
    t1_type = pltpu.VMEM((n_out, lines - 2, half, 2 * channels), F32)
    slots_type = pltpu.VMEM((n_frames, lines, half, 4 * channels), BF16)
    operands = (meta, *stats, gain.reshape(1, channels), shift.reshape(1, channels), t0,
                weight.reshape(9, 3, channels, channels))
    t1, slots, sums = pl.pallas_call(
        functools.partial(time1_kernel, n_out=n_out, **settings),
        out_shape=(t1_type, slots_type, jax.ShapeDtypeStruct((-(-2 * n_out // 8) * 8, channels), F32)),
        in_specs=[SMEM] + [VMEM] * 8,
        out_specs=(VMEM, VMEM, VMEM),
        compiler_params=params(26),
        cost_estimate=cost(30e9),
        name="time1",
    )(*operands)

    def outer_lines():
        return pl.pallas_call(
            functools.partial(time1_edge_kernel, **settings),
            out_shape=(t1_type, slots_type),
            in_specs=[SMEM] + [VMEM] * 10,
            out_specs=(VMEM, VMEM),
            input_output_aliases={9: 0, 10: 1},
            compiler_params=params(26),
            cost_estimate=cost(8e9),
            name="time1_edge",
        )(*operands, t1, slots)[0]

    return sums, outer_lines


def time2_kernel(
    meta, s0, s1, s2, s3, gain, shift, bias, ts, t0s, w_ref, outv, slots, rowf,
    *, count, per_group, n_blocks,
):
    frames, lines, half, _ = slots.shape
    own = lines - 2
    channels = gain.shape[1]
    width = 2 * half
    scale, move = half_affine((s0, s1, s2, s3), frames, gain[...], shift[...], count, per_group)
    first_line = meta[0] * own - 1

    def norm(k, r):
        line = first_line + r
        inside = (line >= 0) & (line < n_blocks * own) & (meta[1] >= k)
        even = half_silu(ts[k, r, :, 0:channels], scale[k : k + 1], move[k : k + 1])
        odd = half_silu(ts[k, r, :, channels : 2 * channels], scale[k : k + 1], move[k : k + 1])
        spread_columns(slots.at[k], r, 0, jnp.where(inside, even, 0.0), jnp.where(inside, odd, 0.0), channels)

    part_lines = own // 2
    blocks = [(0, 0), (0, part_lines)]

    def finish(k, first, acc):
        acc = acc.reshape(part_lines, half, 2 * channels)
        for r in range(part_lines):
            for parity in range(2):
                at = (2 + first + r) * width + parity * half
                value = acc[r, :, parity * channels : (parity + 1) * channels] + bias[...]
                rowf[first + r, pl.ds(parity, half, stride=2), :] = value + t0s[at : at + half, 0:channels]
            outv[0, first + r] = rowf[first + r].astype(BF16)

    ahead = Ahead(block_order(blocks, part_lines), norm)
    clip_blocks(slots, w_ref, blocks, part_lines, ahead, finish, 4)


def time2(meta, stats, gain, shift, bias, t1, t0, weight, n_blocks):
    frames, lines, half, _ = t1.shape
    own = lines - 2
    channels = gain.shape[0]
    count = float(n_blocks * own * 2 * half * (channels // GROUPS))
    return pl.pallas_call(
        functools.partial(time2_kernel, count=count, per_group=channels // GROUPS, n_blocks=n_blocks),
        out_shape=jax.ShapeDtypeStruct((1, own, 2 * half, channels), BF16),
        in_specs=[SMEM] + [VMEM] * 10,
        out_specs=VMEM,
        scratch_shapes=[
            pltpu.VMEM((frames, lines, half, 4 * channels), BF16),
            pltpu.VMEM((own, 2 * half, channels), F32),
        ],
        compiler_params=params(24),
        cost_estimate=cost(12e9),
        name="time2",
    )(meta, *stats, gain.reshape(1, channels), shift.reshape(1, channels), bias.reshape(1, channels), t1, t0,
      weight.reshape(9, 3, channels, channels))


def turned(block, axis, distance):
    count = lax.axis_size(axis)
    return lax.ppermute(block, axis, [(i, (i + distance) % count) for i in range(count)])


def swapped(block, first):
    count = lax.axis_size("rows")
    route = {i: i for i in range(count)}
    for i in range(first, count - 1, 2):
        route[i], route[i + 1] = i + 1, i
    return lax.ppermute(block, "rows", list(route.items()))


def from_all(block):
    parts = [block]
    for distance in range(1, lax.axis_size("rows")):
        parts.append(turned(block, "rows", distance))
    return parts


def window(
    video, norm1_gain, norm1_shift, conv1_weight, conv1_bias, norm2_gain, norm2_shift, conv2_weight, conv2_bias,
    out_gain, out_shift, out_weight, out_bias, quant_weight, quant_bias, time_in_weight, time_in_bias,
    tnorm1_gain, tnorm1_shift, time1_weight, tnorm2_gain, tnorm2_shift, time2_weight, time2_bias,
):
    x = video[0]
    own, width, _ = x.shape
    half = width // 2
    n_blocks = lax.axis_size("rows")
    meta = jnp.stack([lax.axis_index("rows"), lax.axis_index("frames")]).astype(jnp.int32)
    channels = x.shape[2]
    weight = conv1_weight.reshape(3, 3 * channels, channels)
    x, near, far, sums = input_sums(meta, x, 2)
    stats = from_all(sums)
    far = swapped(far, 1)
    near = swapped(near, 0)
    xp, sums, outer_lines = conv1(meta, stats, norm1_gain, norm1_shift, conv1_bias, x, (near, far), weight, n_blocks)
    stats = from_all(sums)
    h = outer_lines()
    y, sums = conv2(meta, stats, norm2_gain, norm2_shift, conv2_bias, h, xp, conv2_weight, n_blocks)
    part, to_up, to_low = head(
        meta, from_all(sums), out_gain, out_shift, y, out_weight, out_bias, quant_weight, quant_bias, n_blocks, 4
    )
    above = turned(to_low, "rows", 1)
    below = turned(to_up, "rows", -1)
    size = -(-((own + 6) * width) // LANES) * LANES
    row = lax.axis_index("rows")
    above = jnp.where(row > 0, above, 0.0)
    below = jnp.where(row < n_blocks - 1, below, 0.0)
    latent = (
        jnp.pad(part, ((0, 0), (2 * width, size))) [:, :size]
        + jnp.pad(above, ((0, 0), (0, size - 4 * width)))
        + jnp.pad(below, ((0, 0), ((own + 2) * width, size - (own + 6) * width)))
    ).astype(BF16)
    n_frames = lax.axis_size("frames")
    latents = lax.all_to_all(jnp.broadcast_to(latent[None], (n_frames,) + latent.shape), "frames", 0, 0)
    t0, sums = lift(meta, time_in_weight, time_in_bias, latents, own, half, 7, 5)
    sums, outer_lines = time1(meta, from_all(sums), tnorm1_gain, tnorm1_shift, t0, time1_weight, n_blocks, own, half, 5, 3)
    stats = from_all(sums)
    t1 = outer_lines()
    return time2(meta, stats, tnorm2_gain, tnorm2_shift, time2_bias, t1, t0, time2_weight, n_blocks)


def solution(mesh):
    return jax.shard_map(
        window,
        mesh=mesh,
        in_specs=(P("frames", "rows", None, None),) + (P(),) * 23,
        out_specs=P("frames", "rows", None, None),
        check_vma=False,
    )
```

```python
import functools

import jax
import jax.numpy as jnp
from jax import lax
from jax.experimental import pallas as pl
from jax.experimental.pallas import tpu as pltpu
from jax.sharding import PartitionSpec as P


GROUPS = 32
EPS = 1e-06
LATENT_SCALE = 0.13025
LANES = 128
F32 = jnp.float32
BF16 = jnp.bfloat16

HBM = pl.BlockSpec(memory_space=pltpu.HBM)
VMEM = pl.BlockSpec(memory_space=pltpu.VMEM)
SMEM = pl.BlockSpec(memory_space=pltpu.SMEM)


def in_hbm(array):
    return pltpu.with_memory_space_constraint(array, pltpu.HBM)


def params(mib=48):
    return pltpu.CompilerParams(vmem_limit_bytes=mib * 1024 * 1024)


def cost(flops):
    return pl.CostEstimate(flops=int(flops), transcendentals=0, bytes_accessed=0)


def lane_groups(values, size):
    lane = lax.broadcasted_iota(jnp.int32, values.shape, 1)
    step = 1
    while step < size:
        up = pltpu.roll(values, step, 1)
        down = pltpu.roll(values, LANES - step, 1)
        values = values + jnp.where((lane & step) != 0, up, down)
        step *= 2
    return values


def half_affine(parts, rows, gain, shift, count, per_group):
    total = parts[0][...]
    for part in parts[1:]:
        total = total + part[...]
    total = lane_groups(total, per_group) * (1.0 / count)
    mean = total[0:rows]
    variance = total[rows : 2 * rows] - mean * mean
    scale = lax.rsqrt(variance + EPS) * gain
    return 0.5 * scale, 0.5 * (shift - mean * scale)


def as_row(block):
    return jnp.concatenate([block[k : k + 1, :] for k in range(block.shape[0])], axis=1)


def half_silu(values, scale, shift):
    t = values * scale + shift
    return t * jnp.tanh(t) + t


def put_sums(out_ref, first, second, rows):
    for k in range(rows):
        lanes = slice(k * LANES, (k + 1) * LANES)
        out_ref[k : k + 1, :] = first[:, lanes]
        out_ref[rows + k : rows + k + 1, :] = second[:, lanes]


def spread_columns(slots, row, at, even, odd, channels):
    half, width = even.shape
    index = lax.broadcasted_iota(jnp.int32, (half, width), 0)
    before = jnp.where(index == 0, 0.0, pltpu.roll(odd, 1, 0))
    after = jnp.where(index == half - 1, 0.0, pltpu.roll(even, half - 1, 0))
    for slot, piece in enumerate((before, even, odd, after)):
        slots[row, :, slot * channels + at : slot * channels + at + width] = piece.astype(BF16)


def input_sums_kernel(meta, x_hbm, x_ref, near_ref, far_ref, out_ref, sems):
    lines, width, channels = x_ref.shape
    halo = near_ref.shape[0]
    rows = channels // LANES
    even = (meta[0] & 1) == 0
    copies = [pltpu.make_async_copy(x_hbm.at[r], x_ref.at[r], sems.at[r]) for r in range(lines)]
    for copy in copies:
        copy.start()
    first = [jnp.zeros((8, LANES), F32) for _ in range(rows)]
    second = list(first)
    for r in range(lines):
        copies[r].wait()
        for k in range(rows):
            v = x_ref[r, :, k * LANES : (k + 1) * LANES].astype(F32).reshape(width // 8, 8, LANES)
            first[k] = first[k] + v.sum(0)
            second[k] = second[k] + (v * v).sum(0)
    for r in range(halo):
        top, bottom = x_ref[r], x_ref[lines - halo + r]
        near_ref[r] = jnp.where(even, bottom, top)
        far_ref[r] = jnp.where(even, top, bottom)
    for k in range(rows):
        out_ref[k : k + 1, :] = first[k].sum(0, keepdims=True)
        out_ref[rows + k : rows + k + 1, :] = second[k].sum(0, keepdims=True)


def input_sums(meta, x, halo):
    lines, width, channels = x.shape
    edge = pltpu.VMEM((halo, width, channels), BF16)
    return pl.pallas_call(
        input_sums_kernel,
        out_shape=(
            pltpu.VMEM(x.shape, BF16),
            edge,
            edge,
            jax.ShapeDtypeStruct((2 * channels // LANES, LANES), F32),
        ),
        in_specs=[SMEM, HBM],
        out_specs=(VMEM,) * 4,
        scratch_shapes=[pltpu.SemaphoreType.DMA((lines,))],
        compiler_params=params(8),
        cost_estimate=cost(6e9),
        name="input_sums",
    )(meta, in_hbm(x))


def norm_line(slots, row, read, scale, move, inside, channels, keep=None):
    for at in range(0, channels, LANES):
        cols = slice(at, at + LANES)
        even, odd = read(at // LANES, cols)
        if keep is not None:
            keep[0, :, cols] = even.astype(BF16)
            keep[1, :, cols] = odd.astype(BF16)
        even = jnp.where(inside, half_silu(even, scale[:, cols], move[:, cols]), 0.0)
        odd = jnp.where(inside, half_silu(odd, scale[:, cols], move[:, cols]), 0.0)
        spread_columns(slots, row, at, even, odd, channels)


def block_conv(slots, weights, firsts, lines, channels, between=()):
    half = slots.shape[1]
    acc = None
    for i in range(3):
        parts = [
            slots[f + i : f + i + lines, :, p * channels : (p + 3) * channels].reshape(lines * half, 3 * channels)
            for p in range(2)
            for f in firsts
        ]
        part = jnp.dot(jnp.concatenate(parts, axis=0), weights[i], preferred_element_type=F32)
        acc = part if acc is None else acc + part
        if i < len(between):
            between[i]()
    return acc.reshape(2, len(firsts) * lines, half, channels)


class Sums:
    def __init__(self, channels):
        self.channels = channels
        self.first = jnp.zeros((8, channels), F32)
        self.second = jnp.zeros((8, channels), F32)

    def add(self, line):
        line = line.reshape(-1, 8, self.channels)
        self.first = self.first + line.sum(0)
        self.second = self.second + (line * line).sum(0)

    def put(self, out_ref, base=None):
        rows = self.channels // LANES
        put_sums(out_ref, self.first.sum(0, keepdims=True), self.second.sum(0, keepdims=True), rows)
        if base is not None:
            out_ref[...] += base[...]


def conv1_kernel(
    s0, s1, s2, s3, gain, shift, bias, x_ref, w_ref, h_ref, xp_ref, slots, stats_ref, rowf,
    *, halo, count, per_group,
):
    own, width, channels = x_ref.shape
    half = width // 2
    scale, move = half_affine((s0, s1, s2, s3), channels // LANES, gain[...], shift[...], count, per_group)
    scale, move = as_row(scale), as_row(move)
    offset = bias[...].reshape(1, 1, 1, channels)

    def norm(r):
        def read(chunk, cols):
            rowf[r, chunk] = x_ref[r, :, cols].astype(F32)
            return rowf[r, chunk, pl.ds(0, half, stride=2), :], rowf[r, chunk, pl.ds(1, half, stride=2), :]

        norm_line(slots, halo + r, read, scale, move, True, channels, xp_ref.at[r])

    sums = Sums(channels)
    norm(0)
    norm(1)
    for b in range(0, own - 2, 2):
        lines = [functools.partial(norm, r) for r in (range(2, 6) if b == 0 else range(b + 4, b + 6)) if r < own]
        acc = block_conv(slots, w_ref, [halo + b], 2, channels, lines[:2]) + offset
        for line in lines[2:]:
            line()
        for r in range(2):
            for p in range(2):
                h_ref[halo + b + r, p] = acc[p, r]
                sums.add(acc[p, r])
    sums.put(stats_ref)


def conv1_edge_kernel(
    meta, s0, s1, s2, s3, gain, shift, bias, near_ref, far_ref, base, w_ref, h_in, slots_in, h_ref, slots, *rest,
    distance, count, per_group, n_blocks,
):
    rowf = rest[-1]
    halo, width, channels = near_ref.shape
    half = width // 2
    lines = slots.shape[0]
    even_block = (meta[0] & 1) == 0
    scale, move = half_affine((s0, s1, s2, s3), channels // LANES, gain[...], shift[...], count, per_group)
    scale, move = as_row(scale), as_row(move)
    offset = bias[...].reshape(1, 1, 1, channels)

    def norm(above, r, inside, at, spare):
        def read(chunk, cols):
            near, far = near_ref[r, :, cols].astype(F32), far_ref[r, :, cols].astype(F32)
            rowf[spare, chunk] = jnp.where(even_block == above, far, near)
            return rowf[spare, chunk, pl.ds(0, half, stride=2), :], rowf[spare, chunk, pl.ds(1, half, stride=2), :]

        norm_line(slots, at, read, scale, move, inside, channels)

    top, bottom = halo - 1 - distance, lines - halo + distance
    norm(True, top, meta[0] > 0, top, 0)
    norm(False, distance, meta[0] < n_blocks - 1, bottom, 1)
    places = (top, bottom - 2)
    acc = block_conv(slots, w_ref, places, 1, channels) + offset
    sums = Sums(channels)
    for k, place in enumerate(places):
        for p in range(2):
            h_ref[place, p] = acc[p, k]
            if distance == 0:
                sums.add(acc[p, k])
    if distance == 0:
        sums.put(rest[0], base)


def conv1(meta, stats, gain, shift, bias, x, halos, weight, n_blocks):
    near, far = halos
    own, width, channels = x.shape
    halo = near.shape[0]
    lines = own + 2 * halo
    half = width // 2
    rows = channels // LANES
    settings = dict(count=float(n_blocks * own * width * (channels // GROUPS)), per_group=channels // GROUPS)
    gain, shift, bias = gain.reshape(rows, LANES), shift.reshape(rows, LANES), bias.reshape(1, channels)
    h_type = pltpu.VMEM((lines - 2, 2, half, channels), F32)
    slots_type = pltpu.VMEM((lines, half, 4 * channels), BF16)
    stats_type = jax.ShapeDtypeStruct((2 * rows, LANES), F32)
    h, xp, slots, base = pl.pallas_call(
        functools.partial(conv1_kernel, halo=halo, **settings),
        out_shape=(
            h_type,
            pltpu.VMEM((own, 2, half, channels), BF16),
            slots_type,
            stats_type,
        ),
        in_specs=[VMEM] * 9,
        out_specs=(VMEM,) * 4,
        scratch_shapes=[pltpu.VMEM((own, channels // LANES, width, LANES), F32)],
        compiler_params=params(26),
        cost_estimate=cost(25e9),
        name="conv1",
    )(*stats, gain, shift, bias, x, weight)

    def edge(distance, h, slots):
        return pl.pallas_call(
            functools.partial(conv1_edge_kernel, distance=distance, n_blocks=n_blocks, **settings),
            out_shape=(h_type, slots_type) + ((stats_type,) if distance == 0 else ()),
            in_specs=[SMEM] + [VMEM] * 13,
            out_specs=(VMEM,) * (3 if distance == 0 else 2),
            scratch_shapes=[pltpu.VMEM((2, channels // LANES, width, LANES), F32)],
            input_output_aliases={12: 0, 13: 1},
            compiler_params=params(26),
            cost_estimate=cost(10e9),
        )(meta, *stats, gain, shift, bias, near, far, base, weight, h, slots)

    h, slots, sums = edge(0, h, slots)
    return xp, sums, lambda: edge(1, h, slots)[0]


def conv2_kernel(
    meta, s0, s1, s2, s3, gain, shift, bias, hs, xs, wv, y_ref, stats_ref, slots,
    *, count, per_group, n_blocks,
):
    lines, _, _, channels = hs.shape
    own = lines - 2
    scale, move = half_affine((s0, s1, s2, s3), channels // LANES, gain[...], shift[...], count, per_group)
    scale, move = as_row(scale), as_row(move)
    offset = bias[...].reshape(1, 1, 1, channels)

    def norm(r):
        inside = True
        if r == 0:
            inside = meta[0] > 0
        if r == lines - 1:
            inside = meta[0] < n_blocks - 1
        norm_line(slots, r, lambda chunk, cols: (hs[r, 0, :, cols], hs[r, 1, :, cols]), scale, move, inside, channels)

    sums = Sums(channels)
    norm(0)
    norm(1)
    for b in range(0, own, 2):
        ahead = [functools.partial(norm, r) for r in (range(2, 6) if b == 0 else range(b + 4, b + 6)) if r < lines]
        acc = block_conv(slots, wv, [b], 2, channels, ahead[:2]) + offset
        for line in ahead[2:]:
            line()
        for r in range(2):
            for p in range(2):
                value = acc[p, r] + xs[b + r, p].astype(F32)
                y_ref[b + r, p] = value
                sums.add(value)
    sums.put(stats_ref)


def conv2(meta, stats, gain, shift, bias, h, xp, weight, n_blocks):
    lines, _, half, channels = h.shape
    own = lines - 2
    rows = channels // LANES
    count = float(n_blocks * own * 2 * half * (channels // GROUPS))
    return pl.pallas_call(
        functools.partial(conv2_kernel, count=count, per_group=channels // GROUPS, n_blocks=n_blocks),
        out_shape=(
            pltpu.VMEM((own, 2, half, channels), F32),
            jax.ShapeDtypeStruct((2 * rows, LANES), F32),
        ),
        in_specs=[SMEM] + [VMEM] * 10,
        out_specs=(VMEM, VMEM),
        scratch_shapes=[pltpu.VMEM((lines, half, 4 * channels), BF16)],
        compiler_params=params(26),
        cost_estimate=cost(30e9),
        name="conv2",
    )(meta, *stats, gain.reshape(rows, LANES), shift.reshape(rows, LANES), bias.reshape(1, channels), h, xp,
      weight.reshape(3, 3 * channels, channels))


def column_shift(values, tap, half):
    size = values.shape[1]
    lane = lax.broadcasted_iota(jnp.int32, values.shape, 1) % (2 * half)
    even = lane < half
    if tap == 0:
        moved = jnp.where(even, pltpu.roll(values, size - (half - 1), 1), pltpu.roll(values, half, 1))
        return jnp.where(lane == 0, 0.0, moved)
    moved = jnp.where(even, pltpu.roll(values, size - half, 1), pltpu.roll(values, half - 1, 1))
    return jnp.where(lane == 2 * half - 1, 0.0, moved)


def head_kernel(
    meta, s0, s1, s2, s3, gain, shift, w_ref, b_ref, q_ref, qb_ref, ys, part_ref, up_ref, low_ref, act,
    *, count, per_group, n_blocks, n_send,
):
    own, _, half, channels = ys.shape
    width = 2 * half
    scale, move = half_affine((s0, s1, s2, s3), channels // LANES, gain[...], shift[...], count, per_group)
    scale, move = as_row(scale), as_row(move)

    for r in range(own):
        for parity in range(2):
            for at in range(0, channels, LANES):
                cols = slice(at, at + LANES)
                act[r, parity, :, cols] = half_silu(ys[r, parity, :, cols], scale[:, cols], move[:, cols]).astype(BF16)
    flat = act[...].reshape(own * width, channels)
    taps = lax.dot_general(w_ref[...], flat, (((1,), (1,)), ((), ())), preferred_element_type=F32)
    size = part_ref.shape[1]
    moments_n = taps.shape[0] // 9
    spare = jnp.zeros((moments_n, size - own * width), F32)
    total = None
    for i in range(3):
        piece = None
        for j in range(3):
            at = (3 * i + j) * moments_n
            one = taps[at : at + moments_n]
            one = one if j == 1 else column_shift(one, j, half)
            piece = one if piece is None else piece + one
        piece = jnp.concatenate([piece, spare], axis=1)
        if i < 2:
            piece = pltpu.roll(piece, (2 - i) * width, 1)
        total = piece if total is None else total + piece
    lane = lax.broadcasted_iota(jnp.int32, (1, size), 1)
    own_lane = (lane >= width) & (lane < (own + 1) * width)
    latents = []
    for c in range(q_ref.shape[0]):
        value, offset = None, qb_ref[c]
        for o in range(moments_n):
            term = total[o : o + 1, :] * q_ref[c, o]
            value = term if value is None else value + term
            offset = offset + b_ref[o] * q_ref[c, o]
        latents.append(LATENT_SCALE * (value + jnp.where(own_lane, offset, 0.0)))
    latent = jnp.concatenate(latents, axis=0)
    keep = ((lane >= width) | (meta[0] > 0)) & ((lane < (own + 1) * width) | (meta[0] < n_blocks - 1))
    part_ref[...] = jnp.where(keep, latent, 0.0)
    up_ref[...] = latent[:, : n_send * width]
    low_ref[...] = pltpu.roll(latent, size - (own + 2 - n_send) * width, 1)[:, : n_send * width]


def head(meta, stats, gain, shift, y, weight, bias, quant_weight, quant_bias, n_blocks, n_send):
    own, _, half, channels = y.shape
    width = 2 * half
    rows = channels // LANES
    moments, latents = quant_weight.shape
    count = float(n_blocks * own * width * (channels // GROUPS))
    size = -(-((own + 2) * width) // LANES) * LANES
    taps = weight.transpose(0, 1, 3, 2).reshape(9 * moments, channels)
    return pl.pallas_call(
        functools.partial(head_kernel, count=count, per_group=channels // GROUPS, n_blocks=n_blocks, n_send=n_send),
        out_shape=(
            jax.ShapeDtypeStruct((latents, size), F32),
            jax.ShapeDtypeStruct((latents, n_send * width), F32),
            jax.ShapeDtypeStruct((latents, n_send * width), F32),
        ),
        in_specs=[SMEM] + [VMEM] * 7 + [SMEM] * 3 + [VMEM],
        out_specs=(VMEM, VMEM, VMEM),
        scratch_shapes=[pltpu.VMEM((own, 2, half, channels), BF16)],
        compiler_params=params(12),
        cost_estimate=cost(10e9),
        name="head",
    )(meta, *stats, gain.reshape(rows, LANES), shift.reshape(rows, LANES), taps, bias, quant_weight.T, quant_bias, y)


def lift_kernel(meta, w_ref, bias_ref, latents, t0_ref, stats_ref, stack, patches, weights, *, own, half, n_frames, n_out):
    width = 2 * half
    out_lines = own + 4
    pixels = out_lines * width
    depth, size = stack.shape
    each = latents.shape[1]
    channels = bias_ref.shape[1]
    for s in range(n_frames):
        frame = meta[1] - (n_frames - 1 - s)
        value = latents[jnp.maximum(frame, 0)].astype(F32)
        stack[s * each : (s + 1) * each, :] = jnp.where(frame >= 0, value, 0.0)
    frames = stack[...]
    patches[9 * depth :, :] = jnp.zeros_like(patches[9 * depth :, :])
    weights[...] = jnp.zeros_like(weights)
    for j in range(3):
        moved = frames if j == 1 else column_shift(frames, j, half)
        for i in range(3):
            piece = moved if i == 0 else pltpu.roll(moved, size - i * width, 1)
            at = (3 * i + j) * depth
            patches[at : at + depth, :] = piece[:, :pixels]
            for t in range(3):
                tap = w_ref[9 * t + 3 * i + j].astype(F32)
                for g in range(n_out):
                    row = at + (n_frames - 3 - g + t) * each
                    weights[row : row + each, g * channels : (g + 1) * channels] = tap
    lhs = jnp.transpose(patches[...], (1, 0)).astype(BF16)
    for start in range(0, n_out, 2):
        pair = slice(start * channels, min(start + 2, n_out) * channels)
        values = jnp.dot(lhs, weights[:, pair].astype(BF16), preferred_element_type=F32)
        for g in range(start, min(start + 2, n_out)):
            value = values[:, (g - start) * channels : (g - start + 1) * channels] + bias_ref[...]
            t0_ref[:, g * channels : (g + 1) * channels] = value
            mine = value[2 * width : (2 + own) * width].reshape(-1, 8, channels)
            stats_ref[g : g + 1, :] = mine.sum(0).sum(0, keepdims=True)
            stats_ref[n_out + g : n_out + g + 1, :] = (mine * mine).sum(0).sum(0, keepdims=True)


def lift(meta, weight, bias, latents, own, half, n_frames, n_out):
    _, each, size = latents.shape
    channels = bias.shape[0]
    pixels = (own + 4) * 2 * half
    stat_rows = -(-2 * n_out // 8) * 8
    depth = -(-9 * n_frames * each // 256) * 256
    return pl.pallas_call(
        functools.partial(lift_kernel, own=own, half=half, n_frames=n_frames, n_out=n_out),
        out_shape=(
            pltpu.VMEM((pixels, n_out * channels), F32),
            jax.ShapeDtypeStruct((stat_rows, channels), F32),
        ),
        in_specs=[SMEM] + [VMEM] * 3,
        out_specs=(VMEM, VMEM),
        scratch_shapes=[
            pltpu.VMEM((n_frames * each, size), F32),
            pltpu.VMEM((depth, pixels), F32),
            pltpu.VMEM((depth, n_out * channels), F32),
        ],
        compiler_params=params(20),
        cost_estimate=cost(8e9),
        name="lift",
    )(meta, weight.reshape(27, each, channels), bias.reshape(1, channels), latents)


def pair_weights(w_ref, tap):
    first, second, third = (w_ref[tap, j] for j in range(3))
    none = jnp.zeros_like(first)
    rows = ((first, none), (second, first), (third, second), (none, third))
    return jnp.concatenate([jnp.concatenate(row, axis=1) for row in rows], axis=0)


class Ahead:
    def __init__(self, order, emit):
        self.order, self.emit, self.done = list(dict.fromkeys(order)), emit, set()

    def need(self, items):
        while not self.done.issuperset(items):
            self.more(1)

    def more(self, count):
        for _ in range(min(count, len(self.order))):
            item = self.order.pop(0)
            self.emit(*item)
            self.done.add(item)


def clip_blocks(slots, w_ref, blocks, lines, ahead, finish, pace):
    half, depth = slots.shape[2], slots.shape[3]
    for k, first in blocks:
        acc = None
        for t in range(3):
            frame = k + 2 - t
            ahead.need([(frame, r) for r in range(first, first + lines + 2)])
            for i in range(3):
                lhs = slots[frame, first + i : first + i + lines].reshape(lines * half, depth)
                part = jnp.dot(lhs, pair_weights(w_ref, 3 * t + i), preferred_element_type=F32)
                acc = part if acc is None else acc + part
            ahead.more(pace)
        finish(k, first, acc)


def block_order(blocks, lines):
    return [(k + 2 - t, r) for k, first in blocks for t in range(3) for r in range(first, first + lines + 2)]


def time1_line(ts, slots, meta, scale, move, n_blocks, own):
    half, depth = slots.shape[2], slots.shape[3]
    channels = depth // 4
    width = 2 * half

    def norm(k, r):
        line = meta[0] * own - 2 + r
        inside = meta[1] >= k
        if r < 2 or r >= own + 2:
            inside = inside & (line >= 0) & (line < n_blocks * own)
        at = r * width
        cols = slice(k * channels, (k + 1) * channels)
        even = half_silu(ts[at : at + half, cols], scale[k : k + 1], move[k : k + 1])
        odd = half_silu(ts[at + half : at + width, cols], scale[k : k + 1], move[k : k + 1])
        spread_columns(slots.at[k], r, 0, jnp.where(inside, even, 0.0), jnp.where(inside, odd, 0.0), channels)

    return norm


def time1_kernel(
    meta, s0, s1, s2, s3, gain, shift, ts, w_ref, t1v, slots, stats_ref, *, count, per_group, n_blocks, own, n_out,
):
    frames, _, half, _ = slots.shape
    channels = gain.shape[1]
    scale, move = half_affine((s0, s1, s2, s3), frames, gain[...], shift[...], count, per_group)
    norm = time1_line(ts, slots, meta, scale, move, n_blocks, own)
    part_lines = own // 2
    blocks = [(k, first) for first in (1, 1 + part_lines) for k in reversed(range(n_out))]
    sums = [[jnp.zeros((8, 2 * channels), F32)] * 2 for _ in range(n_out)]

    def finish(k, first, acc):
        t1v[k, first : first + part_lines] = acc.reshape(part_lines, half, 2 * channels)
        mine = acc.reshape(-1, 8, 2 * channels)
        sums[k] = [sums[k][0] + mine.sum(0), sums[k][1] + (mine * mine).sum(0)]

    ahead = Ahead(block_order(blocks, part_lines), norm)
    clip_blocks(slots, w_ref, blocks, part_lines, ahead, finish, 4)
    for k in range(n_out):
        for at, value in enumerate(sums[k]):
            value = value.sum(0, keepdims=True)
            row = at * n_out + k
            stats_ref[row : row + 1, :] = value[:, :channels] + value[:, channels:]


def time1_edge_kernel(
    meta, s0, s1, s2, s3, gain, shift, ts, w_ref, t1_in, slots_in, t1v, slots, *, count, per_group, n_blocks, own,
):
    frames, lines, half, _ = slots.shape
    n_out = t1v.shape[0]
    scale, move = half_affine((s0, s1, s2, s3), frames, gain[...], shift[...], count, per_group)
    norm = time1_line(ts, slots, meta, scale, move, n_blocks, own)
    ends = (0, lines - 1)
    ahead = Ahead([(k + 2 - t, r) for t in range(3) for k in range(n_out) for r in ends], norm)
    places = [(k, first) for k in range(n_out) for first in (0, lines - 3)]
    acc = None
    for t in range(3):
        ahead.need([(k + 2 - t, r) for k in range(n_out) for r in ends])
        for i in range(3):
            lhs = jnp.concatenate([slots[k + 2 - t, first + i] for k, first in places], axis=0)
            part = jnp.dot(lhs, pair_weights(w_ref, 3 * t + i), preferred_element_type=F32)
            acc = part if acc is None else acc + part
        ahead.more(2)
    for at, (k, first) in enumerate(places):
        t1v[k, first] = acc[at * half : (at + 1) * half]


def time1(meta, stats, gain, shift, t0, weight, n_blocks, own, half, n_frames, n_out):
    channels = gain.shape[0]
    lines = own + 4
    settings = dict(
        count=float(n_blocks * own * 2 * half * (channels // GROUPS)),
        per_group=channels // GROUPS,
        n_blocks=n_blocks,
        own=own,
    )
    t1_type = pltpu.VMEM((n_out, lines - 2, half, 2 * channels), F32)
    slots_type = pltpu.VMEM((n_frames, lines, half, 4 * channels), BF16)
    operands = (meta, *stats, gain.reshape(1, channels), shift.reshape(1, channels), t0,
                weight.reshape(9, 3, channels, channels))
    t1, slots, sums = pl.pallas_call(
        functools.partial(time1_kernel, n_out=n_out, **settings),
        out_shape=(t1_type, slots_type, jax.ShapeDtypeStruct((-(-2 * n_out // 8) * 8, channels), F32)),
        in_specs=[SMEM] + [VMEM] * 8,
        out_specs=(VMEM, VMEM, VMEM),
        compiler_params=params(26),
        cost_estimate=cost(30e9),
        name="time1",
    )(*operands)

    def outer_lines():
        return pl.pallas_call(
            functools.partial(time1_edge_kernel, **settings),
            out_shape=(t1_type, slots_type),
            in_specs=[SMEM] + [VMEM] * 10,
            out_specs=(VMEM, VMEM),
            input_output_aliases={9: 0, 10: 1},
            compiler_params=params(26),
            cost_estimate=cost(8e9),
            name="time1_edge",
        )(*operands, t1, slots)[0]

    return sums, outer_lines


def time2_kernel(
    meta, s0, s1, s2, s3, gain, shift, bias, ts, t0s, w_ref, outv, slots, rowf,
    *, count, per_group, n_blocks,
):
    frames, lines, half, _ = slots.shape
    own = lines - 2
    channels = gain.shape[1]
    width = 2 * half
    scale, move = half_affine((s0, s1, s2, s3), frames, gain[...], shift[...], count, per_group)
    first_line = meta[0] * own - 1

    def norm(k, r):
        line = first_line + r
        inside = (line >= 0) & (line < n_blocks * own) & (meta[1] >= k)
        even = half_silu(ts[k, r, :, 0:channels], scale[k : k + 1], move[k : k + 1])
        odd = half_silu(ts[k, r, :, channels : 2 * channels], scale[k : k + 1], move[k : k + 1])
        spread_columns(slots.at[k], r, 0, jnp.where(inside, even, 0.0), jnp.where(inside, odd, 0.0), channels)

    part_lines = own // 2
    blocks = [(0, 0), (0, part_lines)]

    def finish(k, first, acc):
        acc = acc.reshape(part_lines, half, 2 * channels)
        for r in range(part_lines):
            for parity in range(2):
                at = (2 + first + r) * width + parity * half
                value = acc[r, :, parity * channels : (parity + 1) * channels] + bias[...]
                rowf[first + r, pl.ds(parity, half, stride=2), :] = value + t0s[at : at + half, 0:channels]
            outv[0, first + r] = rowf[first + r].astype(BF16)

    ahead = Ahead(block_order(blocks, part_lines), norm)
    clip_blocks(slots, w_ref, blocks, part_lines, ahead, finish, 4)


def time2(meta, stats, gain, shift, bias, t1, t0, weight, n_blocks):
    frames, lines, half, _ = t1.shape
    own = lines - 2
    channels = gain.shape[0]
    count = float(n_blocks * own * 2 * half * (channels // GROUPS))
    return pl.pallas_call(
        functools.partial(time2_kernel, count=count, per_group=channels // GROUPS, n_blocks=n_blocks),
        out_shape=jax.ShapeDtypeStruct((1, own, 2 * half, channels), BF16),
        in_specs=[SMEM] + [VMEM] * 10,
        out_specs=VMEM,
        scratch_shapes=[
            pltpu.VMEM((frames, lines, half, 4 * channels), BF16),
            pltpu.VMEM((own, 2 * half, channels), F32),
        ],
        compiler_params=params(24),
        cost_estimate=cost(12e9),
        name="time2",
    )(meta, *stats, gain.reshape(1, channels), shift.reshape(1, channels), bias.reshape(1, channels), t1, t0,
      weight.reshape(9, 3, channels, channels))


def turned(block, axis, distance):
    count = lax.axis_size(axis)
    return lax.ppermute(block, axis, [(i, (i + distance) % count) for i in range(count)])


def swapped(block, first):
    count = lax.axis_size("rows")
    route = {i: i for i in range(count)}
    for i in range(first, count - 1, 2):
        route[i], route[i + 1] = i + 1, i
    return lax.ppermute(block, "rows", list(route.items()))


def from_all(block):
    count = lax.axis_size("rows")
    parts = [block]
    for distance in range(1, count):
        if count & (count - 1) == 0:
            parts.append(lax.ppermute(block, "rows", [(i, i ^ distance) for i in range(count)]))
        else:
            parts.append(turned(block, "rows", distance))
    return parts


def window(
    video, norm1_gain, norm1_shift, conv1_weight, conv1_bias, norm2_gain, norm2_shift, conv2_weight, conv2_bias,
    out_gain, out_shift, out_weight, out_bias, quant_weight, quant_bias, time_in_weight, time_in_bias,
    tnorm1_gain, tnorm1_shift, time1_weight, tnorm2_gain, tnorm2_shift, time2_weight, time2_bias,
):
    x = video[0]
    own, width, _ = x.shape
    half = width // 2
    n_blocks = lax.axis_size("rows")
    meta = jnp.stack([lax.axis_index("rows"), lax.axis_index("frames")]).astype(jnp.int32)
    channels = x.shape[2]
    weight = conv1_weight.reshape(3, 3 * channels, channels)
    x, near, far, sums = input_sums(meta, x, 2)
    stats = from_all(sums)
    far = swapped(far, 1)
    near = swapped(near, 0)
    xp, sums, outer_lines = conv1(meta, stats, norm1_gain, norm1_shift, conv1_bias, x, (near, far), weight, n_blocks)
    stats = from_all(sums)
    h = outer_lines()
    y, sums = conv2(meta, stats, norm2_gain, norm2_shift, conv2_bias, h, xp, conv2_weight, n_blocks)
    part, to_up, to_low = head(
        meta, from_all(sums), out_gain, out_shift, y, out_weight, out_bias, quant_weight, quant_bias, n_blocks, 4
    )
    above = turned(to_low, "rows", 1)
    below = turned(to_up, "rows", -1)
    size = -(-((own + 6) * width) // LANES) * LANES
    row = lax.axis_index("rows")
    above = jnp.where(row > 0, above, 0.0)
    below = jnp.where(row < n_blocks - 1, below, 0.0)
    latent = (
        jnp.pad(part, ((0, 0), (2 * width, size))) [:, :size]
        + jnp.pad(above, ((0, 0), (0, size - 4 * width)))
        + jnp.pad(below, ((0, 0), ((own + 2) * width, size - (own + 6) * width)))
    ).astype(BF16)
    n_frames = lax.axis_size("frames")
    latents = lax.all_to_all(jnp.broadcast_to(latent[None], (n_frames,) + latent.shape), "frames", 0, 0)
    t0, sums = lift(meta, time_in_weight, time_in_bias, latents, own, half, 7, 5)
    sums, outer_lines = time1(meta, from_all(sums), tnorm1_gain, tnorm1_shift, t0, time1_weight, n_blocks, own, half, 5, 3)
    stats = from_all(sums)
    t1 = outer_lines()
    return time2(meta, stats, tnorm2_gain, tnorm2_shift, time2_bias, t1, t0, time2_weight, n_blocks)


def solution(mesh):
    return jax.shard_map(
        window,
        mesh=mesh,
        in_specs=(P("frames", "rows", None, None),) + (P(),) * 23,
        out_specs=P("frames", "rows", None, None),
        check_vma=False,
    )
```
